256 devices in a mesh: seq: 8 (over x, core), dom: 32 (over z, y).
Axes of the slice: x: 4, y: 4, z: 8, core: 2. Of those that a mesh axis runs over, the one named last changes fastest.
Arguments:
- observed: bfloat16 [40, 88], P('seq'), parts along dimension 0, may hold values from -18 to 18
- latent_noise: float32 [4, 128, 32768], P(None, None, ('seq', 'dom')), parts along dimension 2, may hold values from -6 to 6
- w_hidden: bfloat16 [4096, 1024], replicated, may hold values from -0.1875 to 0.1875
- w_latent: bfloat16 [4096, 128], replicated, may hold values from -0.5 to 0.5
- w_frame: bfloat16 [88, 4096], replicated, may hold values from -0.625 to 0.625
- gate_bias: float32 [4096], replicated, may hold values from -3 to 3
- w_prior: bfloat16 [256, 1024], replicated, may hold values from -0.1875 to 0.1875
- w_emit: bfloat16 [88, 128], replicated, may hold values from -0.09375 to 0.09375
- w_emit_hidden: bfloat16 [88, 1024], replicated, may hold values from -0.046875 to 0.046875
- block_source: int32 [24, 32], P('seq'), parts along dimension 0, may hold values from 0 to 31, as said below
- inner_offset: int32 [24, 4096], P('seq'), parts along dimension 0, may hold values from 0 to 127
- resample_flags: int32 [3], replicated, may hold values from 0 to 1, as said below
Outputs:
- final_hidden: bfloat16 [1024, 32768], P(None, ('seq', 'dom')), parts along dimension 1
- fivo_bound: float32 [8], P('seq'), parts along dimension 0
The draws below stay inside these ranges and needn't reach their ends.
There are 8 independent parts, one for each index of `seq`. The reference program is written for one: setup_inputs(seed, part) draws one part's arguments, and reference() takes and returns one part's arrays. A program takes and returns all parts, laid end to end along the dimension named above; an argument that names none is the same for every part. Nothing has to cross between parts.
Inputs may be any that keep to these rules, and one draw needn't show every extreme that they name: block_source[t, j] differs from j by at most 1 for every transition t and block j; in every draw some block takes the particles of the block 1 places before it and some those of the block 1 places after it. `resample_flags`: at least one entry is 1 and at least one is 0.
All inputs are finite; a program needn't handle non-finite values.
Results may differ from the reference program's by a relative error of at most 0.0023.
The reference program's roundings to bfloat16 on the way (of `hidden`, `cell_state` and `latent`) count: a program that leaves them out, or rounds other values in their place, can miss the bound.
Values may be sent and summed in bfloat16 or wider, within the bound.
No kernel may reach another device: no remote copies, remote signals or barrier semaphores. Data moves between devices by JAX's collectives and lax.ppermute only.
A program may use at most 64 MiB of HBM per device.

```python
import math
import jax
import jax.numpy as jnp

H = 1024
Z = 128
X = 88
BLK = 128
REACH = 1
NB_DEV = 1
STEPS = 4
RESAMPLES = 3
NBLK = 32
NPART = 4096


def draw_observed(key, part):
    key_rows, key_signs = jax.random.split(key)
    frame_rows = jnp.clip(0.8 * jax.random.normal(key_rows, (STEPS + 1, X), jnp.float32), -4.8, 4.8)
    return frame_rows.astype(jnp.bfloat16)


def draw_latent_noise(key, part):
    values = jnp.clip(jax.random.normal(key, (STEPS, Z, NPART), jnp.float32), -6.0, 6.0)
    return values


def draw_block_source(key, part):
    shifts = jax.random.randint(key, (RESAMPLES, NBLK), -REACH, REACH + 1)
    shifts = shifts.at[:, NB_DEV].set(-REACH)
    shifts = shifts.at[:, 3 * NB_DEV - 1].set(REACH)
    places = jnp.arange(NBLK, dtype=jnp.int32)[None, :] + shifts
    return jnp.clip(places, 0, NBLK - 1).astype(jnp.int32)


def draw_resample_flags(key, part):
    key_bits, key_one, key_zero = jax.random.split(key, 3)
    chosen = jax.random.randint(key_bits, (RESAMPLES,), 0, 2)
    ones_at = jax.random.randint(key_one, (), 0, RESAMPLES)
    zero_at = (ones_at + 1 + jax.random.randint(key_zero, (), 0, RESAMPLES - 1)) % RESAMPLES
    chosen = chosen.at[ones_at].set(1).at[zero_at].set(0)
    return chosen.astype(jnp.int32)


def plant(array, own_key, least, high):
    index_at = [jax.random.randint(jax.random.fold_in(own_key, axis), (), 0, length) for axis, length in enumerate(array.shape)]
    main_axis = array.shape.index(max(array.shape))
    neighbour = index_at[:main_axis] + [(index_at[main_axis] + 1) % array.shape[main_axis]] + index_at[main_axis + 1:]
    return array.at[tuple(index_at)].set(least).at[tuple(neighbour)].set(high)


def noise(own_key, dims, scale, bound, kind=jnp.bfloat16):
    drawn = scale * jax.random.normal(own_key, dims, jnp.float32)
    return jnp.clip(drawn, min=-bound, max=bound).astype(kind)


def setup_inputs(seed: int = 0, part: int = 0) -> dict:
    streams_of = jax.random.split(jax.random.key(seed), 13)
    own_keys = jax.random.split(jax.random.fold_in(streams_of[12], part), 13)
    return {
        "observed": draw_observed(jax.random.fold_in(jax.random.fold_in(streams_of[12], part), 71), part),
        "latent_noise": draw_latent_noise(jax.random.fold_in(jax.random.fold_in(streams_of[12], part), 71), part),
        "w_hidden": noise(streams_of[2], (4 * H, H), H ** -0.5, 0.1875),
        "w_latent": noise(streams_of[3], (4 * H, Z), Z ** -0.5, 0.5),
        "w_frame": noise(streams_of[4], (X, 4 * H), X ** -0.5, 0.625),
        "gate_bias": noise(streams_of[5], (4 * H,), 0.5, 3.0, jnp.float32),
        "w_prior": noise(streams_of[6], (2 * Z, H), H ** -0.5, 0.1875),
        "w_emit": noise(streams_of[7], (X, Z), (32 * Z) ** -0.5, 0.09375),
        "w_emit_hidden": noise(streams_of[8], (X, H), (16 * H) ** -0.5, 0.046875),
        "block_source": draw_block_source(jax.random.fold_in(jax.random.fold_in(streams_of[12], part), 71), part),
        "inner_offset": plant(jax.random.randint(own_keys[10], (RESAMPLES, NPART), 0, BLK), jax.random.fold_in(own_keys[10], 1), 0, BLK - 1).astype(jnp.int32),
        "resample_flags": draw_resample_flags(jax.random.fold_in(streams_of[12], 71), part),
    }


def cell_update(gate_pre, cell_state, width):
    in_gate = jax.nn.sigmoid(gate_pre[:width])
    forget = jax.nn.sigmoid(gate_pre[width:2 * width])
    cand_gate = jnp.tanh(gate_pre[2 * width:3 * width])
    out_gate = jax.nn.sigmoid(gate_pre[3 * width:])
    fresh = forget * cell_state.astype(jnp.float32) + in_gate * cand_gate
    hidden = (out_gate * jnp.tanh(fresh)).astype(jnp.bfloat16)
    return hidden, fresh.astype(jnp.bfloat16)


def particle_step(hidden, latent, cell_state, frame_row, moment_noise, target_row, w_hidden, w_latent, gate_bias, w_prior, w_emit, w_emit_hidden):
    gate_pre = jnp.dot(w_hidden, hidden, preferred_element_type=jnp.float32)
    gate_pre = gate_pre + jnp.dot(w_latent, latent, preferred_element_type=jnp.float32)
    gate_pre = gate_pre + (frame_row + gate_bias)[:, None]
    hidden, cell_state = cell_update(gate_pre, cell_state, w_hidden.shape[1])
    prior_out = jnp.dot(w_prior, hidden, preferred_element_type=jnp.float32)
    zdim = w_latent.shape[1]
    latent = (prior_out[:zdim] + jnp.exp(0.5 * jnp.tanh(prior_out[zdim:])) * moment_noise).astype(jnp.bfloat16)
    predicted = jnp.dot(w_emit, latent, preferred_element_type=jnp.float32)
    predicted = predicted + jnp.dot(w_emit_hidden, hidden, preferred_element_type=jnp.float32)
    target = target_row.astype(jnp.float32)[:, None]
    increment = jnp.sum(predicted * (target - 0.5 * predicted), axis=0)
    return hidden, latent, cell_state, increment


def reference(observed, latent_noise, w_hidden, w_latent, w_frame, gate_bias, w_prior, w_emit, w_emit_hidden, block_source, inner_offset, resample_flags):
    width = w_hidden.shape[1]
    zdim = w_latent.shape[1]
    particles = latent_noise.shape[2]
    frames = jnp.dot(observed[:STEPS], w_frame, preferred_element_type=jnp.float32)
    hidden = jnp.zeros((width, particles), jnp.bfloat16)
    cell_state = jnp.zeros((width, particles), jnp.bfloat16)
    latent = jnp.zeros((zdim, particles), jnp.bfloat16)
    log_weight = jnp.zeros((particles,), jnp.float32)
    bound_sum = jnp.zeros((), jnp.float32)
    log_count = math.log(particles)
    for moment in range(STEPS):
        hidden, latent, cell_state, increment = particle_step(hidden, latent, cell_state, frames[moment], latent_noise[moment], observed[moment + 1], w_hidden, w_latent, gate_bias, w_prior, w_emit, w_emit_hidden)
        log_weight = log_weight + increment
        if moment < STEPS - 1:
            do_move = resample_flags[moment] == 1
            level_now = jax.nn.logsumexp(log_weight) - log_count
            bound_sum = bound_sum + jnp.where(do_move, level_now, jnp.zeros_like(level_now))
            ancestor = (block_source[moment][:, None] * BLK + inner_offset[moment].reshape(-1, BLK)).reshape(-1).astype(jnp.int32)
            hidden = jnp.where(do_move, hidden[:, ancestor], hidden)
            latent = jnp.where(do_move, latent[:, ancestor], latent)
            cell_state = jnp.where(do_move, cell_state[:, ancestor], cell_state)
            log_weight = jnp.where(do_move, jnp.zeros_like(log_weight), log_weight)
    bound_sum = bound_sum + jax.nn.logsumexp(log_weight) - log_count
    return hidden, bound_sum.reshape(1)
```

```python
from functools import partial
import math

import jax
import jax.numpy as jnp
from jax import lax
from jax.experimental import pallas as pl
from jax.experimental.pallas import tpu as pltpu
from jax.sharding import PartitionSpec as P

BLK = 128
CHUNKS = 8
F32 = jnp.float32
BF16 = jnp.bfloat16


def sigmoid(x):
    return 0.5 * jnp.tanh(0.5 * x) + 0.5


def mm(a, b):
    return jnp.dot(a, b, preferred_element_type=F32)


def three_parts(x):
    hi = x.astype(BF16)
    rest = x - hi.astype(F32)
    mid = rest.astype(BF16)
    return hi, mid, (rest - mid.astype(F32)).astype(BF16)


def emission(w_emit, w_emit_hidden, latent, hidden, target):
    predicted = mm(w_emit, latent) + mm(w_emit_hidden, hidden)
    return jnp.sum(predicted * (target - 0.5 * predicted), axis=0, keepdims=True)


def start_kernel(
    obs_ref, noise_ref, wh_hbm, wl_ref, wf_ref, bias_ref, wp_ref, we_ref, weh_ref,
    wx_ref, ext_ref, c0_ref, prior_ref, inc_ref,
    wh, tmp, square, gates, sems,
):
    width = wh.shape[2]
    rows = width // CHUNKS
    nx = wf_ref.shape[0]
    copies = [
        pltpu.make_async_copy(
            wh_hbm.at[:, pl.ds(c * rows, rows)], wh.at[:, pl.ds(c * rows, rows)], sems.at[c]
        )
        for c in range(CHUNKS)
    ]
    for copy in copies:
        copy.start()
    lane = lax.broadcasted_iota(jnp.int32, (BLK, BLK), 1)
    square[...] = jnp.where((lane >= nx) & (lane < nx + 3), 1.0, 0.0)
    square[0:5, 0:nx] = obs_ref[...].astype(F32)
    obs_cols = square[...].T
    steps = ext_ref.shape[0]
    ext = []
    for t in range(steps + 1):
        ext.append(jnp.broadcast_to(obs_cols[:, t : t + 1], (BLK, BLK)))
    row = lax.broadcasted_iota(jnp.int32, (BLK, BLK), 0)
    for t in range(steps):
        value = ext[t]
        if t == 1:
            value = jnp.where((row >= nx + 3) & (row < nx + 6), 1.0, value)
        ext_ref[t] = value.astype(BF16)
    tmp[0:nx, :] = wf_ref[...].astype(F32)
    tmp[nx:, :] = jnp.zeros((BLK - nx, tmp.shape[1]), F32)
    for k, part in enumerate(three_parts(bias_ref[...])):
        tmp[nx + k : nx + k + 1, :] = part.astype(F32)
    ext0 = ext[0].astype(BF16)
    for r in range(4 * width // BLK):
        cols = tmp[:, r * BLK : (r + 1) * BLK].T
        wx_ref[r * BLK : (r + 1) * BLK, BLK:] = cols.astype(BF16)
        wx_ref[r * BLK : (r + 1) * BLK, :BLK] = wl_ref[r * BLK : (r + 1) * BLK, :]
    in_gate = sigmoid(mm(wx_ref[0:width, BLK:], ext0))
    cand = jnp.tanh(mm(wx_ref[2 * width : 3 * width, BLK:], ext0))
    fresh = in_gate * cand
    hidden = (sigmoid(mm(wx_ref[3 * width :, BLK:], ext0)) * jnp.tanh(fresh)).astype(BF16)
    c0_ref[...] = fresh.astype(BF16)
    gates[...] = hidden
    prior = mm(wp_ref[...], hidden)
    mean, scale = prior[:BLK], jnp.exp(0.5 * jnp.tanh(prior[BLK:]))
    prior_ref[0] = mean
    prior_ref[1] = scale
    latent = (mean + scale * noise_ref[0]).astype(BF16)
    inc = emission(we_ref[...], weh_ref[...], latent, hidden, ext[1][:nx])
    inc_ref[...] = jnp.broadcast_to(inc, inc_ref.shape)
    lane_r = lax.broadcasted_iota(jnp.int32, (rows, BLK), 1)
    for c in range(CHUNKS):
        copies[c].wait()
        for g in range(4):
            at = g * width + c * rows
            shared = mm(wh[g, c * rows : (c + 1) * rows, :], gates[...])
            hi, mid, lo = (p.astype(F32) for p in three_parts(shared))
            old = wx_ref[at : at + rows, BLK:].astype(F32)
            new = jnp.where(
                lane_r == nx + 3, hi, jnp.where(lane_r == nx + 4, mid, jnp.where(lane_r == nx + 5, lo, old))
            )
            wx_ref[at : at + rows, BLK:] = new.astype(BF16)


def main_kernel(
    flags, source, me_ref,
    off_ref, noise_ref, m1_ref, p1_ref, m2_ref, p2_ref, wh_hbm, wx_ref, ext_ref, c0_ref, prior_ref, inc_ref,
    wp_ref, we_ref, weh_ref,
    out_ref, part_ref,
    wh, h1, c1, l1, h2, c2, l2, inc1, sems,
):
    width = wh.shape[2]
    rows = width // CHUNKS
    nx = we_ref.shape[0]
    copies = [
        pltpu.make_async_copy(
            wh_hbm.at[:, pl.ds(c * rows, rows)], wh.at[:, pl.ds(c * rows, rows)], sems.at[c]
        )
        for c in range(CHUNKS)
    ]
    for copy in copies:
        copy.start()
    me = me_ref[0]
    f0, f1, f2 = flags[0] == 1, flags[1] == 1, flags[2] == 1
    last = off_ref.shape[1] // BLK - 1

    def block(flag, t, at):
        return jnp.where(flag, jnp.clip(source[t, at], 0, last), at)

    def offsets(t, at):
        start = pl.multiple_of(at * BLK, BLK)
        return jnp.broadcast_to(off_ref[t : t + 1, pl.ds(start, BLK)], (8, BLK))

    def take(x, idx):
        idx = jnp.broadcast_to(idx[0:1], x.shape)
        return jnp.take_along_axis(x, idx, axis=1, mode="promise_in_bounds")

    own = lax.broadcasted_iota(jnp.int32, (8, BLK), 1)
    bx2 = block(f2, 2, me)
    cx2 = jnp.where(f2, offsets(2, me), own)
    bx1 = block(f1, 1, bx2)
    cx1 = jnp.where(f1, take(offsets(1, bx2), cx2), cx2)
    bx0 = block(f0, 0, bx1)
    cx0 = jnp.where(f0, take(offsets(0, bx1), cx1), cx1)
    by1 = block(f1, 1, me)
    cy1 = jnp.where(f1, offsets(1, me), own)
    by0 = block(f0, 0, by1)
    cy0 = jnp.where(f0, take(offsets(0, by1), cy1), cy1)
    bw0 = block(f0, 0, me)
    cw0 = jnp.where(f0, offsets(0, me), own)

    def noise(t, at, cols):
        d = at - me
        value = noise_ref[t]
        value = jnp.where(d == -1, m1_ref[t].astype(F32), value)
        value = jnp.where(d == 1, p1_ref[t].astype(F32), value)
        if t < 2:
            value = jnp.where(d == -2, m2_ref[t].astype(F32), value)
            value = jnp.where(d == 2, p2_ref[t].astype(F32), value)
        return take(value, cols)

    def first_latent(at, cols):
        return (prior_ref[0] + prior_ref[1] * noise(0, at, cols)).astype(BF16)

    def gate_rows(g, c):
        return slice(g * width + c * rows, g * width + (c + 1) * rows)

    def cell(pre, cell_state):
        fresh = sigmoid(pre[1]) * cell_state + sigmoid(pre[0]) * jnp.tanh(pre[2])
        return (sigmoid(pre[3]) * jnp.tanh(fresh)).astype(BF16), fresh.astype(BF16)

    def step_one(slot, at, cols):
        ext = jnp.concatenate([first_latent(at, cols), ext_ref[1]], axis=0)
        for c in range(CHUNKS):
            here = slice(c * rows, (c + 1) * rows)
            pre = [mm(wx_ref[gate_rows(g, c), :], ext) for g in range(4)]
            h1[slot, here, :], c1[slot, here, :] = cell(pre, c0_ref[here, :].astype(F32))

    def latents(hidden, value):
        prior = mm(wp_ref[...], hidden)
        return (prior[:BLK] + jnp.exp(0.5 * jnp.tanh(prior[BLK:])) * value).astype(BF16)

    def increment(t, latent, hidden):
        target = ext_ref[t + 1, 0:nx, :].astype(F32)
        return emission(we_ref[...], weh_ref[...], latent, hidden, target)

    step_one(0, bw0, cw0)
    step_one(1, bx0, cx0)
    l1[0] = latents(h1[0], noise_ref[1])
    l1[1] = latents(h1[1], noise(1, bx1, cx1))
    inc1 = increment(1, l1[0], h1[0])

    @pl.when(f1 & f2)
    def _():
        step_one(2, by0, cy0)
        l1[2] = latents(h1[2], noise(1, by1, cy1))

    slot = jnp.where(f1, jnp.where(f2, 2, 1), 0)
    hidden = jnp.concatenate([h1[slot], h1[1]], axis=1)
    ext2 = jnp.concatenate([ext_ref[2], ext_ref[2]], axis=1)
    ext = jnp.concatenate([jnp.concatenate([l1[slot], l1[1]], axis=1), ext2], axis=0)
    for c in range(CHUNKS):
        here = slice(c * rows, (c + 1) * rows)
        copies[c].wait()
        pre = [mm(wh[g, here, :], hidden) + mm(wx_ref[gate_rows(g, c), :], ext) for g in range(4)]
        before = jnp.concatenate([c1[slot, here, :], c1[1, here, :]], axis=1).astype(F32)
        h2[here, :], c2[here, :] = cell(pre, before)
    hidden = h2[...]
    value = jnp.concatenate([noise_ref[2], noise(2, bx2, cx2)], axis=1)
    l2[...] = latents(hidden, value)
    inc2 = increment(2, l2[:, :BLK], h2[:, :BLK])

    hidden = h2[:, BLK:]
    ext = jnp.concatenate([l2[:, BLK:], ext_ref[3]], axis=0)
    for c in range(CHUNKS):
        here = slice(c * rows, (c + 1) * rows)
        pre = [mm(wh[g, here, :], hidden) + mm(wx_ref[gate_rows(g, c), :], ext) for g in range(4)]
        out_ref[here, :], _unused = cell(pre, c2[here, BLK:].astype(F32))
    hidden = out_ref[...]
    latent = latents(hidden, noise_ref[3])
    inc3 = increment(3, latent, hidden)

    lane = lax.broadcasted_iota(jnp.int32, (1, BLK), 1)
    weights, line = inc_ref[0:1, :], jnp.zeros((1, BLK), F32)
    for t, (inc, flag) in enumerate(((inc1, f0), (inc2, f1), (inc3, f2), (None, None))):
        peak = jnp.max(weights, axis=1, keepdims=True)
        summed = jnp.sum(jnp.exp(weights - peak), axis=1, keepdims=True)
        line = jnp.where(lane == t, peak, jnp.where(lane == t + 4, summed, line))
        if inc is not None:
            weights = jnp.where(flag, jnp.zeros_like(weights), weights) + inc
    part_ref[...] = jnp.broadcast_to(line[None], part_ref.shape)


def bound_kernel(log_count, flags, part_ref, out_ref):
    pairs = part_ref[...].reshape(part_ref.shape[0], BLK)
    peaks = jnp.max(pairs, axis=0, keepdims=True)
    sums = pltpu.roll(pairs, BLK - 4, 1)
    summed = jnp.sum(sums * jnp.exp(pairs - peaks), axis=0, keepdims=True)
    lane = lax.broadcasted_iota(jnp.int32, (1, BLK), 1)
    used = lane == 3
    for t in range(3):
        used = used | ((lane == t) & (flags[t] == 1))
    levels = peaks + jnp.log(jnp.where(used, summed, 1.0)) - log_count
    out_ref[0] = jnp.sum(jnp.where(used, levels, 0.0))


def spec(space):
    return pl.BlockSpec(memory_space=space)


VM, SM, ANY = pltpu.VMEM, pltpu.SMEM, pl.ANY


def body(
    observed, latent_noise, w_hidden, w_latent, w_frame, gate_bias, w_prior, w_emit, w_emit_hidden,
    block_source, inner_offset, resample_flags,
):
    count = lax.axis_size("dom")
    width = w_hidden.shape[1]
    steps = latent_noise.shape[0]
    sds = jax.ShapeDtypeStruct

    def moved(value, shift):
        pairs = [(i, i + shift) for i in range(count) if 0 <= i + shift < count]
        return lax.ppermute(value, "dom", pairs)

    near, far = latent_noise[:3], latent_noise[:2]
    halos = [moved(near, 1), moved(near, -1), moved(far, 2), moved(far, -2)]
    wh = w_hidden.reshape(4, width, width)
    wx, ext, c0, prior, inc = pl.pallas_call(
        start_kernel,
        name="start",
        out_shape=[
            sds((4 * width, 2 * BLK), BF16),
            sds((steps + 1, BLK, BLK), BF16),
            sds((width, BLK), BF16),
            sds((2, BLK, BLK), F32),
            sds((8, BLK), F32),
        ],
        in_specs=[spec(VM), spec(VM), spec(ANY)] + [spec(VM)] * 6,
        out_specs=[spec(VM)] * 5,
        scratch_shapes=[
            pltpu.VMEM((4, width, width), BF16),
            pltpu.VMEM((BLK, 4 * width), F32),
            pltpu.VMEM((BLK, BLK), F32),
            pltpu.VMEM((width, BLK), BF16),
            pltpu.SemaphoreType.DMA((CHUNKS,)),
        ],
    )(observed, latent_noise, wh, w_latent, w_frame, gate_bias.reshape(1, -1), w_prior, w_emit, w_emit_hidden)
    me = lax.axis_index("dom").astype(jnp.int32).reshape(1)
    hidden, part = pl.pallas_call(
        main_kernel,
        name="main",
        out_shape=[sds((width, BLK), BF16), sds((count, 1, BLK), F32)],
        in_specs=[spec(SM)] * 3 + [spec(VM)] * 6 + [spec(ANY)] + [spec(VM)] * 8,
        out_specs=[spec(VM)] * 2,
        scratch_shapes=[
            pltpu.VMEM((4, width, width), BF16),
            pltpu.VMEM((3, width, BLK), BF16),
            pltpu.VMEM((3, width, BLK), BF16),
            pltpu.VMEM((3, BLK, BLK), BF16),
            pltpu.VMEM((width, 2 * BLK), BF16),
            pltpu.VMEM((width, 2 * BLK), BF16),
            pltpu.VMEM((BLK, 2 * BLK), BF16),
            pltpu.VMEM((8, BLK), F32),
            pltpu.SemaphoreType.DMA((CHUNKS,)),
        ],
    )(
        resample_flags, block_source, me, inner_offset, latent_noise, *halos, wh, wx, ext, c0, prior, inc,
        w_prior, w_emit, w_emit_hidden,
    )
    parts = lax.all_to_all(part, "dom", 0, 0, tiled=True)
    bound = pl.pallas_call(
        partial(bound_kernel, math.log(BLK * count)),
        name="bound",
        out_shape=sds((1,), F32),
        in_specs=[spec(SM), spec(VM)],
        out_specs=spec(SM),
    )(resample_flags, parts)
    return hidden, bound


def solution(mesh):
    in_specs = (
        P("seq", None),
        P(None, None, ("seq", "dom")),
        P(),
        P(),
        P(),
        P(),
        P(),
        P(),
        P(),
        P("seq", None),
        P("seq", None),
        P(),
    )
    out_specs = (P(None, ("seq", "dom")), P("seq"))
    return jax.shard_map(body, mesh=mesh, in_specs=in_specs, out_specs=out_specs, check_vma=False)
```

```python
from functools import partial
import math

import jax
import jax.numpy as jnp
from jax import lax
from jax.experimental import pallas as pl
from jax.experimental.pallas import tpu as pltpu
from jax.sharding import PartitionSpec as P

BLK = 128
CHUNKS = 4
F32 = jnp.float32
BF16 = jnp.bfloat16
VM, SM, ANY = pltpu.VMEM, pltpu.SMEM, pl.ANY


def sigmoid(x):
    return 0.5 * jnp.tanh(0.5 * x) + 0.5


def mm(a, b):
    return jnp.dot(a, b, preferred_element_type=F32)


def mm_rows(a, b):
    return lax.dot_general(a, b, (((1,), (1,)), ((), ())), preferred_element_type=F32)


def three_parts(x):
    hi = x.astype(BF16)
    rest = x - hi.astype(F32)
    mid = rest.astype(BF16)
    return hi, mid, (rest - mid.astype(F32)).astype(BF16)


def column(row):
    return jnp.broadcast_to(row, (BLK, BLK)).T


def start_kernel(
    wh_hbm, obs_ref, noise_ref, wf_ref, bias_ref, wp_ref, we_ref, weh_ref,
    wr_ref, ext_ref, c0_ref, prior_ref, inc_ref,
    wh, tmp, square, sems,
):
    width = c0_ref.shape[0]
    pieces = sems.shape[0]
    rows = 4 * width // pieces
    nx = wf_ref.shape[0]
    copies = [
        pltpu.make_async_copy(wh_hbm.at[pl.ds(c * rows, rows)], wh.at[pl.ds(c * rows, rows)], sems.at[c])
        for c in range(pieces)
    ]
    for copy in copies:
        copy.start()
    lane = lax.broadcasted_iota(jnp.int32, (BLK, BLK), 1)
    row = lax.broadcasted_iota(jnp.int32, (BLK, BLK), 0)
    square[...] = jnp.where((lane >= nx) & (lane < nx + 3), 1.0, 0.0)
    square[0:5, 0:nx] = obs_ref[...].astype(F32)
    frame = mm(square[0:8, 0:nx].astype(BF16), wf_ref[...])[0:1]
    gates = frame + bias_ref[...]
    fresh = sigmoid(gates[:, 0:width]) * jnp.tanh(gates[:, 2 * width : 3 * width])
    hidden = (sigmoid(gates[:, 3 * width :]) * jnp.tanh(fresh)).astype(BF16)
    fresh = fresh.astype(BF16).astype(F32)
    hidden8 = jnp.broadcast_to(hidden.astype(F32), (8, width)).astype(BF16)

    tmp[0:nx, :] = wf_ref[...].astype(F32)
    tmp[nx:, :] = jnp.zeros((BLK - nx, tmp.shape[1]), F32)
    for k, part in enumerate(three_parts(bias_ref[...])):
        tmp[nx + k : nx + k + 1, :] = part.astype(F32)

    obs_cols = square[...].T
    for t in range(1, ext_ref.shape[0]):
        value = jnp.broadcast_to(obs_cols[:, t : t + 1], (BLK, BLK))
        if t == 1:
            target = value[:nx]
            value = jnp.where((row >= nx + 3) & (row < nx + 6), 1.0, value)
        ext_ref[t] = value.astype(BF16)
    for r in range(width // BLK):
        c0_ref[r * BLK : (r + 1) * BLK, :] = column(fresh[:, r * BLK : (r + 1) * BLK]).astype(BF16)
    prior = mm_rows(hidden8, wp_ref[...])[0:1]
    mean = column(prior[:, :BLK])
    scale = column(jnp.exp(0.5 * jnp.tanh(prior[:, BLK:])))
    prior_ref[0] = mean
    prior_ref[1] = scale
    latent = (mean + scale * noise_ref[0]).astype(BF16)
    shared = mm_rows(hidden8, weh_ref[...])[0:1]
    shared = jnp.concatenate([shared, jnp.zeros((1, BLK - nx), F32)], axis=1)
    predicted = mm(we_ref[...], latent) + column(shared)[:nx]
    inc = jnp.sum(predicted * (target - 0.5 * predicted), axis=0, keepdims=True)
    inc_ref[...] = jnp.broadcast_to(inc, inc_ref.shape)
    for c in range(pieces):
        copies[c].wait()
        here = slice(c * rows, (c + 1) * rows)
        moved = mm_rows(hidden8, wh[here, :])[0:1]
        for k, part in enumerate(three_parts(moved)):
            tmp[nx + 3 + k : nx + 4 + k, here] = part.astype(F32)
        for r in range(c * rows // BLK, (c + 1) * rows // BLK):
            wr_ref[r * BLK : (r + 1) * BLK, :] = tmp[:, r * BLK : (r + 1) * BLK].T.astype(BF16)


def take(x, idx):
    idx = jnp.broadcast_to(idx[0:1], x.shape)
    return jnp.take_along_axis(x, idx, axis=1, mode="promise_in_bounds")


def transition(t, source, off_ref, me):
    last = off_ref.shape[1] // BLK - 1
    at = jnp.clip(source[t, me], 0, last)
    start = pl.multiple_of(me * BLK, BLK)
    cols = jnp.where(t == 2, off_ref[2:3, pl.ds(start, BLK)], off_ref[1:2, pl.ds(start, BLK)])
    cols = jnp.where(t == 0, off_ref[0:1, pl.ds(start, BLK)], cols)
    return at - me, jnp.broadcast_to(cols, (8, BLK))


def picked(d, cols, own, before, after):
    value = jnp.where(d == -1, before.astype(F32), jnp.where(d == 1, after.astype(F32), own.astype(F32)))
    return take(value, cols)


def cell(pre, cell_state):
    fresh = sigmoid(pre[1]) * cell_state + sigmoid(pre[0]) * jnp.tanh(pre[2])
    return (sigmoid(pre[3]) * jnp.tanh(fresh)).astype(BF16), fresh.astype(BF16)


class Weights:
    def __init__(self, hbm, vmem, sems):
        wl, wr, wh, wp, weh = hbm
        self.wx, self.wh, self.wp, self.weh = vmem
        width = self.wh.shape[1]
        self.rows = width // CHUNKS
        self.width = width
        pairs = [(wl, self.wx.at[:, pl.ds(0, BLK)]), (wr, self.wx.at[:, pl.ds(BLK, BLK)])]
        pairs += [(wp, self.wp), (weh, self.weh)]
        for c in range(CHUNKS):
            for g in range(4):
                here = pl.ds(g * width + c * self.rows, self.rows)
                pairs.append((wh.at[here], self.wh.at[here]))
        self.copies = [pltpu.make_async_copy(a, b, sems.at[k]) for k, (a, b) in enumerate(pairs)]
        for copy in self.copies:
            copy.start()

    def wait_first(self):
        for k in range(4):
            self.copies[k].wait()

    def wait_chunk(self, c):
        for g in range(4):
            self.copies[4 + 4 * c + g].wait()

    def at(self, g, c):
        start = g * self.width + c * self.rows
        return slice(start, start + self.rows)


def latents(w, hidden, value):
    prior = mm(w.wp[...], hidden)
    return (prior[:BLK] + jnp.exp(0.5 * jnp.tanh(prior[BLK:])) * value).astype(BF16)


def increment(w, we_ref, target, latent, hidden):
    predicted = mm(we_ref[...], latent) + mm(w.weh[...], hidden)
    target = target[: predicted.shape[0], :].astype(F32)
    return jnp.sum(predicted * (target - 0.5 * predicted), axis=0, keepdims=True)


def first_step(w, lat, ext_ref, c0_ref, put):
    sets = lat.shape[1] // BLK
    ext = jnp.concatenate([lat, jnp.concatenate([ext_ref[1]] * sets, axis=1)], axis=0)
    for c in range(CHUNKS):
        here = slice(c * w.rows, (c + 1) * w.rows)
        pre = [mm(w.wx[w.at(g, c), :], ext) for g in range(4)]
        before = c0_ref[here, :].astype(F32)
        put(here, *cell(pre, jnp.concatenate([before] * sets, axis=1)))


def later_step(w, hidden, ext, before, put, wait):
    for c in range(CHUNKS):
        here = slice(c * w.rows, (c + 1) * w.rows)
        if wait:
            w.wait_chunk(c)
        pre = [mm(w.wh[w.at(g, c), :], hidden) + mm(w.wx[w.at(g, c), :], ext) for g in range(4)]
        put(here, *cell(pre, before(here)))


def head(w, flags, source, me, off_ref, noise_ref, m1_ref, p1_ref, ext_ref, c0_ref, prior_ref, we_ref, h1, c1, l1):
    f0, f1 = flags[0] == 1, flags[1] == 1
    t = jnp.where(f0, 0, jnp.where(f1, 1, 2))
    d, cols = transition(t, source, off_ref, me)

    def gathered(k):
        return picked(d, cols, noise_ref[k], m1_ref[k], p1_ref[k])

    g0 = gathered(0)
    value = jnp.concatenate([jnp.where(f0, g0, noise_ref[0]), g0], axis=1)
    mean = jnp.concatenate([prior_ref[0]] * 2, axis=1)
    scale = jnp.concatenate([prior_ref[1]] * 2, axis=1)
    lat = (mean + scale * value).astype(BF16)
    w.wait_first()

    def put(here, hidden, fresh):
        for k in range(2):
            h1[k, here, :] = hidden[:, k * BLK : (k + 1) * BLK]
            c1[k, here, :] = fresh[:, k * BLK : (k + 1) * BLK]

    first_step(w, lat, ext_ref, c0_ref, put)
    value = jnp.concatenate([noise_ref[1], jnp.where(f0, noise_ref[1], gathered(1))], axis=1)
    both = latents(w, jnp.concatenate([h1[0], h1[1]], axis=1), value)
    l1[0] = both[:, :BLK]
    l1[1] = both[:, BLK:]
    inc1 = increment(w, we_ref, ext_ref[2], l1[0], h1[0])
    return lat, inc1, d, cols


def tail(w, slot, value, inc1, flags, noise_ref, ext_ref, inc_ref, we_ref, h1, c1, l1, h2, c2, levels, out_ref, part_ref):
    hidden = jnp.concatenate([h1[slot], h1[1]], axis=1)
    latent = jnp.concatenate([l1[slot], l1[1]], axis=1)
    ext = jnp.concatenate([latent, jnp.concatenate([ext_ref[2]] * 2, axis=1)], axis=0)

    def before(here):
        return jnp.concatenate([c1[slot, here, :], c1[1, here, :]], axis=1).astype(F32)

    def put2(here, hidden, fresh):
        h2[here, :] = hidden
        c2[here, :] = fresh[:, BLK:]

    later_step(w, hidden, ext, before, put2, True)
    latent = latents(w, h2[...], jnp.concatenate([noise_ref[2], value], axis=1))
    ext = jnp.concatenate([latent[:, BLK:], ext_ref[3]], axis=0)

    def put3(here, hidden, fresh):
        out_ref[here, :] = hidden

    later_step(w, h2[:, BLK:], ext, lambda here: c2[here, :].astype(F32), put3, False)
    inc2 = increment(w, we_ref, ext_ref[3], latent[:, :BLK], h2[:, :BLK])
    latent = latents(w, out_ref[...], noise_ref[3])
    inc3 = increment(w, we_ref, ext_ref[4], latent, out_ref[...])
    weights = inc_ref[0:1, :]
    levels[...] = jnp.zeros_like(levels)
    levels[0:1, :] = weights
    for t, inc in enumerate((inc1, inc2, inc3)):
        weights = jnp.where(flags[t] == 1, jnp.zeros_like(weights), weights) + inc
        levels[t + 1 : t + 2, :] = weights
    value = levels[...]
    peak = jnp.max(value, axis=1, keepdims=True)
    summed = jnp.sum(jnp.exp(value - peak), axis=1, keepdims=True)
    row = lax.broadcasted_iota(jnp.int32, (8, BLK), 0)
    lane = lax.broadcasted_iota(jnp.int32, (8, BLK), 1)
    line = jnp.where((row < 4) & (lane == row), peak, jnp.where((row < 4) & (lane == row + 4), summed, 0.0))
    line = jnp.sum(line, axis=0, keepdims=True)
    part_ref[...] = jnp.broadcast_to(line[None], part_ref.shape)


def one_kernel(
    flags, source, me_ref,
    wl, wr, wh, wp, weh,
    off_ref, noise_ref, m1_ref, p1_ref, ext_ref, c0_ref, prior_ref, inc_ref, we_ref,
    out_ref, part_ref,
    wx_v, wh_v, wp_v, weh_v, h1, c1, l1, h2, c2, levels, sems,
):
    w = Weights((wl, wr, wh, wp, weh), (wx_v, wh_v, wp_v, weh_v), sems)
    _, inc1, d, cols = head(
        w, flags, source, me_ref[0], off_ref, noise_ref, m1_ref, p1_ref, ext_ref, c0_ref, prior_ref, we_ref, h1, c1, l1
    )
    g2 = picked(d, cols, noise_ref[2], m1_ref[2], p1_ref[2])
    value = jnp.where(flags[2] == 1, g2, noise_ref[2])
    slot = jnp.where(flags[1] == 1, 1, 0)
    tail(w, slot, value, inc1, flags, noise_ref, ext_ref, inc_ref, we_ref, h1, c1, l1, h2, c2, levels, out_ref, part_ref)


def early_kernel(
    flags, source, me_ref,
    wl, wr, wp, weh,
    off_ref, noise_ref, m1_ref, p1_ref, ext_ref, c0_ref, prior_ref, we_ref,
    h_ref, c_ref, msg_ref, inc_ref,
    wx_v, wp_v, weh_v, h1, c1, l1, sems,
):
    w = Weights.__new__(Weights)
    w.wx, w.wp, w.weh = wx_v, wp_v, weh_v
    w.width = wx_v.shape[0] // 4
    w.rows = w.width // CHUNKS
    pairs = [(wl, wx_v.at[:, pl.ds(0, BLK)]), (wr, wx_v.at[:, pl.ds(BLK, BLK)]), (wp, wp_v), (weh, weh_v)]
    w.copies = [pltpu.make_async_copy(a, b, sems.at[k]) for k, (a, b) in enumerate(pairs)]
    for copy in w.copies:
        copy.start()
    lat, inc1, _, _ = head(
        w, flags, source, me_ref[0], off_ref, noise_ref, m1_ref, p1_ref, ext_ref, c0_ref, prior_ref, we_ref, h1, c1, l1
    )
    h_ref[...] = h1[1]
    c_ref[...] = c1[1]
    msg_ref[0] = lat[:, BLK:]
    msg_ref[1] = l1[1]
    inc_ref[...] = jnp.broadcast_to(inc1, inc_ref.shape)


def late_kernel(
    flags, source, me_ref,
    wl, wr, wh, wp, weh,
    off_ref, noise_ref, m1_ref, p1_ref, ext_ref, c0_ref, inc_ref, we_ref,
    h_ref, c_ref, msg_ref, inc1_ref, mm1_ref, mp1_ref,
    out_ref, part_ref,
    wx_v, wh_v, wp_v, weh_v, h1, c1, l1, h2, c2, levels, sems,
):
    w = Weights((wl, wr, wh, wp, weh), (wx_v, wh_v, wp_v, weh_v), sems)
    f2 = flags[2] == 1
    d, cols = transition(jnp.where(f2, 2, 1), source, off_ref, me_ref[0])
    lat = picked(d, cols, msg_ref[0], mm1_ref[0], mp1_ref[0]).astype(BF16)
    l1[1] = picked(d, cols, msg_ref[1], mm1_ref[1], mp1_ref[1]).astype(BF16)
    l1[0] = msg_ref[1]
    h1[0] = h_ref[...]
    c1[0] = c_ref[...]
    g2 = picked(d, cols, noise_ref[2], m1_ref[2], p1_ref[2])
    value = jnp.where(f2, g2, noise_ref[2])
    w.wait_first()

    def put(here, hidden, fresh):
        h1[1, here, :] = hidden
        c1[1, here, :] = fresh

    first_step(w, lat, ext_ref, c0_ref, put)
    slot = jnp.where(f2, 0, 1)
    inc1 = inc1_ref[0:1, :]
    tail(w, slot, value, inc1, flags, noise_ref, ext_ref, inc_ref, we_ref, h1, c1, l1, h2, c2, levels, out_ref, part_ref)


def bound_kernel(log_count, flags, part_ref, out_ref):
    pairs = part_ref[...].reshape(part_ref.shape[0], BLK)
    peaks = jnp.max(pairs, axis=0, keepdims=True)
    sums = pltpu.roll(pairs, BLK - 4, 1)
    summed = jnp.sum(sums * jnp.exp(pairs - peaks), axis=0, keepdims=True)
    lane = lax.broadcasted_iota(jnp.int32, (1, BLK), 1)
    used = lane == 3
    for t in range(3):
        used = used | ((lane == t) & (flags[t] == 1))
    levels = peaks + jnp.log(jnp.where(used, summed, 1.0)) - log_count
    out_ref[0] = jnp.sum(jnp.where(used, levels, 0.0))


def call(kernel, outs, smem, anys, vmem, scratch, args):
    spaces = [SM] * smem + [ANY] * anys + [VM] * vmem
    return pl.pallas_call(
        kernel,
        name=kernel.__name__,
        out_shape=outs,
        in_specs=[pl.BlockSpec(memory_space=s) for s in spaces],
        out_specs=[pl.BlockSpec(memory_space=VM) for _ in outs],
        scratch_shapes=scratch,
    )(*args)


def body(
    observed, latent_noise, w_hidden, w_latent, w_frame, gate_bias, w_prior, w_emit, w_emit_hidden,
    block_source, inner_offset, resample_flags,
):
    count = lax.axis_size("dom")
    width = w_hidden.shape[1]
    nx = w_emit.shape[0]
    steps = latent_noise.shape[0]
    sds = jax.ShapeDtypeStruct
    dma = pltpu.SemaphoreType.DMA

    def moved(value, shift):
        pairs = [(i, i + shift) for i in range(count) if 0 <= i + shift < count]
        return lax.ppermute(value, "dom", pairs)

    near = latent_noise[:3]
    halos = [moved(near, 1), moved(near, -1)]
    wr, ext, c0, prior, inc = call(
        start_kernel,
        [
            sds((4 * width, BLK), BF16),
            sds((steps + 1, BLK, BLK), BF16),
            sds((width, BLK), BF16),
            sds((2, BLK, BLK), F32),
            sds((8, BLK), F32),
        ],
        0,
        1,
        7,
        [
            pltpu.VMEM((4 * width, width), BF16),
            pltpu.VMEM((BLK, 4 * width), F32),
            pltpu.VMEM((BLK, BLK), F32),
            dma((8,)),
        ],
        (w_hidden, observed, latent_noise, w_frame, gate_bias.reshape(1, -1), w_prior, w_emit, w_emit_hidden),
    )
    me = lax.axis_index("dom").astype(jnp.int32).reshape(1)
    outs = [sds((width, BLK), BF16), sds((count, 1, BLK), F32)]
    states = [
        pltpu.VMEM((2, width, BLK), BF16),
        pltpu.VMEM((2, width, BLK), BF16),
        pltpu.VMEM((2, BLK, BLK), BF16),
    ]
    wx_v, wh_v = pltpu.VMEM((4 * width, 2 * BLK), BF16), pltpu.VMEM((4 * width, width), BF16)
    wp_v, weh_v = pltpu.VMEM(w_prior.shape, BF16), pltpu.VMEM(w_emit_hidden.shape, BF16)
    rest = [
        pltpu.VMEM((width, 2 * BLK), BF16),
        pltpu.VMEM((width, BLK), BF16),
        pltpu.VMEM((8, BLK), F32),
        dma((4 + 4 * CHUNKS,)),
    ]
    scalars = (resample_flags, block_source, me)
    shared = (inner_offset, latent_noise, *halos, ext, c0)

    def once():
        return call(
            one_kernel, outs, 3, 5, 9, [wx_v, wh_v, wp_v, weh_v, *states, *rest],
            (*scalars, w_latent, wr, w_hidden, w_prior, w_emit_hidden, *shared, prior, inc, w_emit),
        )

    def twice():
        h_kept, c_kept, msg, inc1 = call(
            early_kernel,
            [sds((width, BLK), BF16), sds((width, BLK), BF16), sds((2, BLK, BLK), BF16), sds((8, BLK), F32)],
            3, 4, 8, [wx_v, wp_v, weh_v, *states, dma((4,))],
            (*scalars, w_latent, wr, w_prior, w_emit_hidden, *shared, prior, w_emit),
        )
        return call(
            late_kernel, outs, 3, 5, 14, [wx_v, wh_v, wp_v, weh_v, *states, *rest],
            (
                *scalars, w_latent, wr, w_hidden, w_prior, w_emit_hidden, *shared, inc, w_emit,
                h_kept, c_kept, msg, inc1, moved(msg, 1), moved(msg, -1),
            ),
        )

    hidden, part = lax.cond(jnp.sum(resample_flags) == 2, twice, once)
    parts = lax.all_to_all(part, "dom", 0, 0, tiled=True)
    bound = pl.pallas_call(
        partial(bound_kernel, math.log(BLK * count)),
        name="bound",
        out_shape=sds((1,), F32),
        in_specs=[pl.BlockSpec(memory_space=SM), pl.BlockSpec(memory_space=VM)],
        out_specs=pl.BlockSpec(memory_space=SM),
    )(resample_flags, parts)
    return hidden, bound


def solution(mesh):
    in_specs = (
        P("seq", None),
        P(None, None, ("seq", "dom")),
        P(),
        P(),
        P(),
        P(),
        P(),
        P(),
        P(),
        P("seq", None),
        P("seq", None),
        P(),
    )
    out_specs = (P(None, ("seq", "dom")), P("seq"))
    return jax.shard_map(body, mesh=mesh, in_specs=in_specs, out_specs=out_specs, check_vma=False)
```

```python
from functools import partial
import math

import jax
import jax.numpy as jnp
from jax import lax
from jax.experimental import pallas as pl
from jax.experimental.pallas import tpu as pltpu
from jax.sharding import PartitionSpec as P

BLK = 128
CHUNKS = 4
F32 = jnp.float32
BF16 = jnp.bfloat16
VM, SM, ANY = pltpu.VMEM, pltpu.SMEM, pl.ANY


def sigmoid(x):
    return 0.5 * jnp.tanh(0.5 * x) + 0.5


def mm(a, b):
    return jnp.dot(a, b, preferred_element_type=F32)


def mm_rows(a, b):
    return lax.dot_general(a, b, (((1,), (1,)), ((), ())), preferred_element_type=F32)


def three_parts(x):
    hi = x.astype(BF16)
    rest = x - hi.astype(F32)
    mid = rest.astype(BF16)
    return hi, mid, (rest - mid.astype(F32)).astype(BF16)


def column(row):
    return jnp.broadcast_to(row, (BLK, BLK)).T


def start_kernel(
    flags, wh_hbm, obs_ref, noise_ref, wf_ref, bias_ref, wp_ref, we_ref, weh_ref,
    wr_ref, ext_ref, c0_ref, prior_ref, inc_ref, twice_ref,
    wh, tmp, square, sems,
):
    twice_ref[0] = jnp.where(flags[0] + flags[1] + flags[2] == 2, 1, 0)
    width = c0_ref.shape[0]
    pieces = sems.shape[0]
    rows = 4 * width // pieces
    nx = wf_ref.shape[0]
    copies = [
        pltpu.make_async_copy(wh_hbm.at[pl.ds(c * rows, rows)], wh.at[pl.ds(c * rows, rows)], sems.at[c])
        for c in range(pieces)
    ]
    for copy in copies:
        copy.start()
    lane = lax.broadcasted_iota(jnp.int32, (BLK, BLK), 1)
    row = lax.broadcasted_iota(jnp.int32, (BLK, BLK), 0)
    square[...] = jnp.where((lane >= nx) & (lane < nx + 3), 1.0, 0.0)
    square[0:5, 0:nx] = obs_ref[...].astype(F32)
    frame = mm(square[0:8, 0:nx].astype(BF16), wf_ref[...])[0:1]
    gates = frame + bias_ref[...]
    fresh = sigmoid(gates[:, 0:width]) * jnp.tanh(gates[:, 2 * width : 3 * width])
    hidden = (sigmoid(gates[:, 3 * width :]) * jnp.tanh(fresh)).astype(BF16)
    fresh = fresh.astype(BF16).astype(F32)
    hidden8 = jnp.broadcast_to(hidden.astype(F32), (8, width)).astype(BF16)

    tmp[0:nx, :] = wf_ref[...].astype(F32)
    tmp[nx:, :] = jnp.zeros((BLK - nx, tmp.shape[1]), F32)
    for k, part in enumerate(three_parts(bias_ref[...])):
        tmp[nx + k : nx + k + 1, :] = part.astype(F32)

    obs_cols = square[...].T
    for t in range(1, ext_ref.shape[0]):
        value = jnp.broadcast_to(obs_cols[:, t : t + 1], (BLK, BLK))
        if t == 1:
            target = value[:nx]
            value = jnp.where((row >= nx + 3) & (row < nx + 6), 1.0, value)
        ext_ref[t] = value.astype(BF16)
    for r in range(width // BLK):
        c0_ref[r * BLK : (r + 1) * BLK, :] = column(fresh[:, r * BLK : (r + 1) * BLK]).astype(BF16)
    prior = mm_rows(hidden8, wp_ref[...])[0:1]
    mean = column(prior[:, :BLK])
    scale = column(jnp.exp(0.5 * jnp.tanh(prior[:, BLK:])))
    prior_ref[0] = mean
    prior_ref[1] = scale
    latent = (mean + scale * noise_ref[0]).astype(BF16)
    shared = mm_rows(hidden8, weh_ref[...])[0:1]
    shared = jnp.concatenate([shared, jnp.zeros((1, BLK - nx), F32)], axis=1)
    predicted = mm(we_ref[...], latent) + column(shared)[:nx]
    inc = jnp.sum(predicted * (target - 0.5 * predicted), axis=0, keepdims=True)
    inc_ref[...] = jnp.broadcast_to(inc, inc_ref.shape)
    for c in range(pieces):
        copies[c].wait()
        here = slice(c * rows, (c + 1) * rows)
        moved = mm_rows(hidden8, wh[here, :])[0:1]
        for k, part in enumerate(three_parts(moved)):
            tmp[nx + 3 + k : nx + 4 + k, here] = part.astype(F32)
        for r in range(c * rows // BLK, (c + 1) * rows // BLK):
            wr_ref[r * BLK : (r + 1) * BLK, :] = tmp[:, r * BLK : (r + 1) * BLK].T.astype(BF16)


def take(x, idx):
    idx = jnp.broadcast_to(idx[0:1], x.shape)
    return jnp.take_along_axis(x, idx, axis=1, mode="promise_in_bounds")


def transition(t, source, off_ref, me):
    last = off_ref.shape[1] // BLK - 1
    at = jnp.clip(source[t, me], 0, last)
    start = pl.multiple_of(me * BLK, BLK)
    cols = jnp.where(t == 2, off_ref[2:3, pl.ds(start, BLK)], off_ref[1:2, pl.ds(start, BLK)])
    cols = jnp.where(t == 0, off_ref[0:1, pl.ds(start, BLK)], cols)
    d = at - me
    partner = jnp.where(d == 0, 0, jnp.where((d == 1) == (lax.rem(me, 2) == 0), 1, 2))
    return partner, jnp.broadcast_to(cols, (8, BLK))


def picked(partner, cols, own, even, odd):
    value = jnp.where(partner == 1, even.astype(F32), jnp.where(partner == 2, odd.astype(F32), own.astype(F32)))
    return take(value, cols)


def cell(pre, cell_state):
    fresh = sigmoid(pre[1]) * cell_state + sigmoid(pre[0]) * jnp.tanh(pre[2])
    return (sigmoid(pre[3]) * jnp.tanh(fresh)).astype(BF16), fresh.astype(BF16)


class Weights:
    def __init__(self, hbm, vmem, sems):
        wl, wr, wh, wp, weh = hbm
        self.wx, self.wh, self.wp, self.weh = vmem
        width = self.wh.shape[1]
        self.rows = width // CHUNKS
        self.width = width
        pairs = [(wl, self.wx.at[:, pl.ds(0, BLK)]), (wr, self.wx.at[:, pl.ds(BLK, BLK)])]
        pairs += [(wp, self.wp), (weh, self.weh)]
        for c in range(CHUNKS):
            for g in range(4):
                here = pl.ds(g * width + c * self.rows, self.rows)
                pairs.append((wh.at[here], self.wh.at[here]))
        self.copies = [pltpu.make_async_copy(a, b, sems.at[k]) for k, (a, b) in enumerate(pairs)]
        for copy in self.copies:
            copy.start()

    def wait_first(self):
        for k in range(4):
            self.copies[k].wait()

    def wait_chunk(self, c):
        for g in range(4):
            self.copies[4 + 4 * c + g].wait()

    def at(self, g, c):
        start = g * self.width + c * self.rows
        return slice(start, start + self.rows)


def latents(w, hidden, value):
    prior = mm(w.wp[...], hidden)
    return (prior[:BLK] + jnp.exp(0.5 * jnp.tanh(prior[BLK:])) * value).astype(BF16)


def increment(w, we_ref, target, latent, hidden):
    predicted = mm(we_ref[...], latent) + mm(w.weh[...], hidden)
    target = target[: predicted.shape[0], :].astype(F32)
    return jnp.sum(predicted * (target - 0.5 * predicted), axis=0, keepdims=True)


def first_step(w, lat, ext_ref, c0_ref, put):
    sets = lat.shape[1] // BLK
    ext = jnp.concatenate([lat, jnp.concatenate([ext_ref[1]] * sets, axis=1)], axis=0)
    for c in range(CHUNKS):
        here = slice(c * w.rows, (c + 1) * w.rows)
        pre = [mm(w.wx[w.at(g, c), :], ext) for g in range(4)]
        before = c0_ref[here, :].astype(F32)
        put(here, *cell(pre, jnp.concatenate([before] * sets, axis=1)))


def later_step(w, hidden, ext, before, put, wait):
    for c in range(CHUNKS):
        here = slice(c * w.rows, (c + 1) * w.rows)
        if wait:
            w.wait_chunk(c)
        pre = [mm(w.wh[w.at(g, c), :], hidden) + mm(w.wx[w.at(g, c), :], ext) for g in range(4)]
        put(here, *cell(pre, before(here)))


def head(w, flags, source, me, off_ref, noise_ref, m1_ref, p1_ref, ext_ref, c0_ref, prior_ref, we_ref, h1, c1, l1):
    f0, f1 = flags[0] == 1, flags[1] == 1
    t = jnp.where(f0, 0, jnp.where(f1, 1, 2))
    d, cols = transition(t, source, off_ref, me)

    def gathered(k):
        return picked(d, cols, noise_ref[k], m1_ref[k], p1_ref[k])

    g0 = gathered(0)
    value = jnp.concatenate([jnp.where(f0, g0, noise_ref[0]), g0], axis=1)
    mean = jnp.concatenate([prior_ref[0]] * 2, axis=1)
    scale = jnp.concatenate([prior_ref[1]] * 2, axis=1)
    lat = (mean + scale * value).astype(BF16)
    w.wait_first()

    def put(here, hidden, fresh):
        for k in range(2):
            h1[k, here, :] = hidden[:, k * BLK : (k + 1) * BLK]
            c1[k, here, :] = fresh[:, k * BLK : (k + 1) * BLK]

    first_step(w, lat, ext_ref, c0_ref, put)
    value = jnp.concatenate([noise_ref[1], jnp.where(f0, noise_ref[1], gathered(1))], axis=1)
    both = latents(w, jnp.concatenate([h1[0], h1[1]], axis=1), value)
    l1[0] = both[:, :BLK]
    l1[1] = both[:, BLK:]
    inc1 = increment(w, we_ref, ext_ref[2], l1[0], h1[0])
    return lat, inc1, d, cols


def tail(w, slot, value, inc1, flags, noise_ref, ext_ref, inc_ref, we_ref, h1, c1, l1, h2, c2, levels, out_ref, part_ref):
    hidden = jnp.concatenate([h1[slot], h1[1]], axis=1)
    latent = jnp.concatenate([l1[slot], l1[1]], axis=1)
    ext = jnp.concatenate([latent, jnp.concatenate([ext_ref[2]] * 2, axis=1)], axis=0)

    def before(here):
        return jnp.concatenate([c1[slot, here, :], c1[1, here, :]], axis=1).astype(F32)

    def put2(here, hidden, fresh):
        h2[here, :] = hidden
        c2[here, :] = fresh[:, BLK:]

    later_step(w, hidden, ext, before, put2, True)
    latent = latents(w, h2[...], jnp.concatenate([noise_ref[2], value], axis=1))
    ext = jnp.concatenate([latent[:, BLK:], ext_ref[3]], axis=0)

    def put3(here, hidden, fresh):
        out_ref[here, :] = hidden

    later_step(w, h2[:, BLK:], ext, lambda here: c2[here, :].astype(F32), put3, False)
    inc2 = increment(w, we_ref, ext_ref[3], latent[:, :BLK], h2[:, :BLK])
    latent = latents(w, out_ref[...], noise_ref[3])
    inc3 = increment(w, we_ref, ext_ref[4], latent, out_ref[...])
    weights = inc_ref[0:1, :]
    levels[...] = jnp.zeros_like(levels)
    levels[0:1, :] = weights
    for t, inc in enumerate((inc1, inc2, inc3)):
        weights = jnp.where(flags[t] == 1, jnp.zeros_like(weights), weights) + inc
        levels[t + 1 : t + 2, :] = weights
    value = levels[...]
    peak = jnp.max(value, axis=1, keepdims=True)
    summed = jnp.sum(jnp.exp(value - peak), axis=1, keepdims=True)
    row = lax.broadcasted_iota(jnp.int32, (8, BLK), 0)
    lane = lax.broadcasted_iota(jnp.int32, (8, BLK), 1)
    line = jnp.where((row < 4) & (lane == row), peak, jnp.where((row < 4) & (lane == row + 4), summed, 0.0))
    line = jnp.sum(line, axis=0, keepdims=True)
    part_ref[...] = jnp.broadcast_to(line[None], part_ref.shape)


def one_kernel(
    flags, source, me_ref,
    wl, wr, wh, wp, weh,
    off_ref, noise_ref, m1_ref, p1_ref, ext_ref, c0_ref, prior_ref, inc_ref, we_ref,
    out_ref, part_ref,
    wx_v, wh_v, wp_v, weh_v, h1, c1, l1, h2, c2, levels, sems,
):
    w = Weights((wl, wr, wh, wp, weh), (wx_v, wh_v, wp_v, weh_v), sems)
    _, inc1, d, cols = head(
        w, flags, source, me_ref[0], off_ref, noise_ref, m1_ref, p1_ref, ext_ref, c0_ref, prior_ref, we_ref, h1, c1, l1
    )
    g2 = picked(d, cols, noise_ref[2], m1_ref[2], p1_ref[2])
    value = jnp.where(flags[2] == 1, g2, noise_ref[2])
    slot = jnp.where(flags[1] == 1, 1, 0)
    tail(w, slot, value, inc1, flags, noise_ref, ext_ref, inc_ref, we_ref, h1, c1, l1, h2, c2, levels, out_ref, part_ref)


def early_kernel(
    flags, source, me_ref,
    wl, wr, wp, weh,
    off_ref, noise_ref, m1_ref, p1_ref, ext_ref, c0_ref, prior_ref, we_ref,
    h_ref, c_ref, msg_ref, inc_ref,
    wx_v, wp_v, weh_v, h1, c1, l1, sems,
):
    w = Weights.__new__(Weights)
    w.wx, w.wp, w.weh = wx_v, wp_v, weh_v
    w.width = wx_v.shape[0] // 4
    w.rows = w.width // CHUNKS
    pairs = [(wl, wx_v.at[:, pl.ds(0, BLK)]), (wr, wx_v.at[:, pl.ds(BLK, BLK)]), (wp, wp_v), (weh, weh_v)]
    w.copies = [pltpu.make_async_copy(a, b, sems.at[k]) for k, (a, b) in enumerate(pairs)]
    for copy in w.copies:
        copy.start()
    lat, inc1, _, _ = head(
        w, flags, source, me_ref[0], off_ref, noise_ref, m1_ref, p1_ref, ext_ref, c0_ref, prior_ref, we_ref, h1, c1, l1
    )
    h_ref[...] = h1[1]
    c_ref[...] = c1[1]
    msg_ref[0] = lat[:, BLK:]
    msg_ref[1] = l1[1]
    inc_ref[...] = jnp.broadcast_to(inc1, inc_ref.shape)


def late_kernel(
    flags, source, me_ref,
    wl, wr, wh, wp, weh,
    off_ref, noise_ref, m1_ref, p1_ref, ext_ref, c0_ref, inc_ref, we_ref,
    h_ref, c_ref, msg_ref, inc1_ref, mm1_ref, mp1_ref,
    out_ref, part_ref,
    wx_v, wh_v, wp_v, weh_v, h1, c1, l1, h2, c2, levels, sems,
):
    w = Weights((wl, wr, wh, wp, weh), (wx_v, wh_v, wp_v, weh_v), sems)
    f2 = flags[2] == 1
    d, cols = transition(jnp.where(f2, 2, 1), source, off_ref, me_ref[0])
    lat = picked(d, cols, msg_ref[0], mm1_ref[0], mp1_ref[0]).astype(BF16)
    l1[1] = picked(d, cols, msg_ref[1], mm1_ref[1], mp1_ref[1]).astype(BF16)
    l1[0] = msg_ref[1]
    h1[0] = h_ref[...]
    c1[0] = c_ref[...]
    g2 = picked(d, cols, noise_ref[2], m1_ref[2], p1_ref[2])
    value = jnp.where(f2, g2, noise_ref[2])
    w.wait_first()

    def put(here, hidden, fresh):
        h1[1, here, :] = hidden
        c1[1, here, :] = fresh

    first_step(w, lat, ext_ref, c0_ref, put)
    slot = jnp.where(f2, 0, 1)
    inc1 = inc1_ref[0:1, :]
    tail(w, slot, value, inc1, flags, noise_ref, ext_ref, inc_ref, we_ref, h1, c1, l1, h2, c2, levels, out_ref, part_ref)


def bound_kernel(log_count, flags, part_ref, out_ref):
    pairs = part_ref[...].reshape(part_ref.shape[0], BLK)
    peaks = jnp.max(pairs, axis=0, keepdims=True)
    sums = pltpu.roll(pairs, BLK - 4, 1)
    summed = jnp.sum(sums * jnp.exp(pairs - peaks), axis=0, keepdims=True)
    lane = lax.broadcasted_iota(jnp.int32, (1, BLK), 1)
    used = lane == 3
    for t in range(3):
        used = used | ((lane == t) & (flags[t] == 1))
    levels = peaks + jnp.log(jnp.where(used, summed, 1.0)) - log_count
    out_ref[0] = jnp.sum(jnp.where(used, levels, 0.0))


def call(kernel, outs, smem, anys, vmem, scratch, args):
    spaces = [SM] * smem + [ANY] * anys + [VM] * vmem
    return pl.pallas_call(
        kernel,
        name=kernel.__name__,
        out_shape=outs,
        in_specs=[pl.BlockSpec(memory_space=s) for s in spaces],
        out_specs=[pl.BlockSpec(memory_space=SM if o.shape == (1,) else VM) for o in outs],
        scratch_shapes=scratch,
    )(*args)


def body(
    observed, latent_noise, w_hidden, w_latent, w_frame, gate_bias, w_prior, w_emit, w_emit_hidden,
    block_source, inner_offset, resample_flags,
):
    count = lax.axis_size("dom")
    width = w_hidden.shape[1]
    nx = w_emit.shape[0]
    steps = latent_noise.shape[0]
    sds = jax.ShapeDtypeStruct
    dma = pltpu.SemaphoreType.DMA

    def swapped(value, first):
        pairs = [(i, i + 1) for i in range(first, count - 1, 2)]
        return lax.ppermute(value, "dom", pairs + [(b, a) for a, b in pairs])

    def exchanged(value):
        odd = swapped(value, 1)
        return swapped(value, 0), odd

    halos = exchanged(latent_noise)
    wr, ext, c0, prior, inc, moves_twice = call(
        start_kernel,
        [
            sds((4 * width, BLK), BF16),
            sds((steps + 1, BLK, BLK), BF16),
            sds((width, BLK), BF16),
            sds((2, BLK, BLK), F32),
            sds((8, BLK), F32),
            sds((1,), jnp.int32),
        ],
        1,
        1,
        7,
        [
            pltpu.VMEM((4 * width, width), BF16),
            pltpu.VMEM((BLK, 4 * width), F32),
            pltpu.VMEM((BLK, BLK), F32),
            dma((8,)),
        ],
        (resample_flags, w_hidden, observed, latent_noise, w_frame, gate_bias.reshape(1, -1), w_prior, w_emit, w_emit_hidden),
    )
    me = lax.axis_index("dom").astype(jnp.int32).reshape(1)
    outs = [sds((width, BLK), BF16), sds((count, 1, BLK), F32)]
    states = [
        pltpu.VMEM((2, width, BLK), BF16),
        pltpu.VMEM((2, width, BLK), BF16),
        pltpu.VMEM((2, BLK, BLK), BF16),
    ]
    wx_v, wh_v = pltpu.VMEM((4 * width, 2 * BLK), BF16), pltpu.VMEM((4 * width, width), BF16)
    wp_v, weh_v = pltpu.VMEM(w_prior.shape, BF16), pltpu.VMEM(w_emit_hidden.shape, BF16)
    rest = [
        pltpu.VMEM((width, 2 * BLK), BF16),
        pltpu.VMEM((width, BLK), BF16),
        pltpu.VMEM((8, BLK), F32),
        dma((4 + 4 * CHUNKS,)),
    ]
    scalars = (resample_flags, block_source, me)
    shared = (inner_offset, latent_noise, *halos, ext, c0)

    def once():
        return call(
            one_kernel, outs, 3, 5, 9, [wx_v, wh_v, wp_v, weh_v, *states, *rest],
            (*scalars, w_latent, wr, w_hidden, w_prior, w_emit_hidden, *shared, prior, inc, w_emit),
        )

    def twice():
        h_kept, c_kept, msg, inc1 = call(
            early_kernel,
            [sds((width, BLK), BF16), sds((width, BLK), BF16), sds((2, BLK, BLK), BF16), sds((8, BLK), F32)],
            3, 4, 8, [wx_v, wp_v, weh_v, *states, dma((4,))],
            (*scalars, w_latent, wr, w_prior, w_emit_hidden, *shared, prior, w_emit),
        )
        return call(
            late_kernel, outs, 3, 5, 14, [wx_v, wh_v, wp_v, weh_v, *states, *rest],
            (
                *scalars, w_latent, wr, w_hidden, w_prior, w_emit_hidden, *shared, inc, w_emit,
                h_kept, c_kept, msg, inc1, *exchanged(msg),
            ),
        )

    hidden, part = lax.cond(moves_twice[0] == 1, twice, once)
    parts = lax.all_to_all(part, "dom", 0, 0, tiled=True)
    bound = pl.pallas_call(
        partial(bound_kernel, math.log(BLK * count)),
        name="bound",
        out_shape=sds((1,), F32),
        in_specs=[pl.BlockSpec(memory_space=SM), pl.BlockSpec(memory_space=VM)],
        out_specs=pl.BlockSpec(memory_space=SM),
    )(resample_flags, parts)
    return hidden, bound


def solution(mesh):
    in_specs = (
        P("seq", None),
        P(None, None, ("seq", "dom")),
        P(),
        P(),
        P(),
        P(),
        P(),
        P(),
        P(),
        P("seq", None),
        P("seq", None),
        P(),
    )
    out_specs = (P(None, ("seq", "dom")), P("seq"))
    return jax.shard_map(body, mesh=mesh, in_specs=in_specs, out_specs=out_specs, check_vma=False)
```

```python
from functools import partial
import math

import jax
import jax.numpy as jnp
from jax import lax
from jax.experimental import pallas as pl
from jax.experimental.pallas import tpu as pltpu
from jax.sharding import PartitionSpec as P

BLK = 128
CHUNKS = 4
PIECES = 4
F32 = jnp.float32
BF16 = jnp.bfloat16
VM, SM, HBM = pltpu.VMEM, pltpu.SMEM, pltpu.HBM
LIMIT = 8 << 20


def sigmoid(x):
    return 0.5 * jnp.tanh(0.5 * x) + 0.5


def mm(a, b):
    return jnp.dot(a, b, preferred_element_type=F32)


def mm_rows(a, b):
    return lax.dot_general(a, b, (((1,), (1,)), ((), ())), preferred_element_type=F32)


def three_parts(x):
    hi = x.astype(BF16)
    rest = x - hi.astype(F32)
    mid = rest.astype(BF16)
    return hi, mid, (rest - mid.astype(F32)).astype(BF16)


def column(row):
    return jnp.broadcast_to(row, (BLK, BLK)).T


def start_kernel(
    flags, obs_hbm, bias_hbm, wf_hbm, wl_hbm, wp_hbm, weh_hbm, wh_hbm,
    wh, wx_ref, ext_ref, c0_ref, prior_ref, wp, weh, twice_ref,
    wf, tmp, square, obs, bias, sems,
):
    width = c0_ref.shape[0]
    pieces = sems.shape[0] - 6
    rows = 4 * width // pieces
    nx = wf.shape[0]
    pairs = [(obs_hbm, obs), (bias_hbm, bias), (wf_hbm, wf), (wp_hbm, wp), (weh_hbm, weh)]
    pairs += [(wh_hbm.at[pl.ds(c * rows, rows)], wh.at[pl.ds(c * rows, rows)]) for c in range(pieces)]
    pairs += [(wl_hbm, wx_ref.at[:, pl.ds(0, BLK)])]
    copies = [pltpu.make_async_copy(a, b, sems.at[k]) for k, (a, b) in enumerate(pairs)]
    for copy in copies:
        copy.start()
    twice_ref[0] = jnp.where(flags[0] + flags[1] + flags[2] == 2, 1, 0)
    lane = lax.broadcasted_iota(jnp.int32, (BLK, BLK), 1)
    row = lax.broadcasted_iota(jnp.int32, (BLK, BLK), 0)
    for copy in copies[:2]:
        copy.wait()
    square[...] = jnp.where((lane >= nx) & (lane < nx + 3), 1.0, 0.0)
    square[0:5, 0:nx] = obs[...].astype(F32)
    tmp[nx:, :] = jnp.zeros((BLK - nx, tmp.shape[1]), F32)
    for k, part in enumerate(three_parts(bias[...])):
        tmp[nx + k : nx + k + 1, :] = part.astype(F32)
    obs_cols = square[...].T
    for t in range(1, ext_ref.shape[0]):
        value = jnp.broadcast_to(obs_cols[:, t : t + 1], (BLK, BLK))
        if t == 1:
            value = jnp.where((row >= nx + 3) & (row < nx + 6), 1.0, value)
        ext_ref[t] = value.astype(BF16)

    copies[2].wait()
    frame = mm(square[0:8, 0:nx].astype(BF16), wf[...])[0:1]
    gates = frame + bias[...]
    fresh = sigmoid(gates[:, 0:width]) * jnp.tanh(gates[:, 2 * width : 3 * width])
    hidden = (sigmoid(gates[:, 3 * width :]) * jnp.tanh(fresh)).astype(BF16)
    fresh = fresh.astype(BF16).astype(F32)
    hidden8 = jnp.broadcast_to(hidden.astype(F32), (8, width)).astype(BF16)
    for copy in copies[3:5]:
        copy.wait()
    prior = mm_rows(hidden8, wp[...])[0:1]
    shared = mm_rows(hidden8, weh[...])[0:1]
    shared = jnp.concatenate([shared, jnp.zeros((1, BLK - nx), F32)], axis=1)
    tmp[0:nx, :] = wf[...].astype(F32)
    for r in range(width // BLK):
        c0_ref[r * BLK : (r + 1) * BLK, :] = column(fresh[:, r * BLK : (r + 1) * BLK]).astype(BF16)
    prior_ref[0] = column(prior[:, :BLK])
    prior_ref[1] = column(jnp.exp(0.5 * jnp.tanh(prior[:, BLK:])))
    prior_ref[2] = column(shared)
    for c in range(pieces):
        copies[5 + c].wait()
        here = slice(c * rows, (c + 1) * rows)
        moved = mm_rows(hidden8, wh[here, :])[0:1]
        for k, part in enumerate(three_parts(moved)):
            tmp[nx + 3 + k : nx + 4 + k, here] = part.astype(F32)
        for r in range(c * rows // BLK, (c + 1) * rows // BLK):
            wx_ref[r * BLK : (r + 1) * BLK, BLK:] = tmp[:, r * BLK : (r + 1) * BLK].T.astype(BF16)
    copies[-1].wait()


def take(x, idx):
    idx = jnp.broadcast_to(idx[0:1], x.shape)
    return jnp.take_along_axis(x, idx, axis=1, mode="promise_in_bounds")


def transition(t, source, off_ref, me):
    last = off_ref.shape[1] // BLK - 1
    at = jnp.clip(source[t, me], 0, last)
    start = pl.multiple_of(me * BLK, BLK)
    cols = jnp.where(t == 2, off_ref[2:3, pl.ds(start, BLK)], off_ref[1:2, pl.ds(start, BLK)])
    cols = jnp.where(t == 0, off_ref[0:1, pl.ds(start, BLK)], cols)
    d = at - me
    partner = jnp.where(d == 0, 0, jnp.where((d == 1) == (lax.rem(me, 2) == 0), 1, 2))
    return partner, jnp.broadcast_to(cols, (8, BLK))


def picked(partner, cols, own, even, odd):
    value = jnp.where(partner == 1, even.astype(F32), jnp.where(partner == 2, odd.astype(F32), own.astype(F32)))
    return take(value, cols)


def cell(pre, cell_state):
    fresh = sigmoid(pre[1]) * cell_state + sigmoid(pre[0]) * jnp.tanh(pre[2])
    return (sigmoid(pre[3]) * jnp.tanh(fresh)).astype(BF16), fresh.astype(BF16)


class Weights:
    def __init__(self, wx, wh, wp, weh):
        self.wx, self.wh, self.wp, self.weh = wx, wh, wp, weh
        self.width = wx.shape[0] // 4
        self.rows = self.width // CHUNKS

    def at(self, g, c):
        start = g * self.width + c * self.rows
        return slice(start, start + self.rows)


def latents(w, hidden, value):
    prior = mm(w.wp[...], hidden)
    return (prior[:BLK] + jnp.exp(0.5 * jnp.tanh(prior[BLK:])) * value).astype(BF16)


def increment(w, we_ref, target, latent, hidden):
    predicted = mm(we_ref[...], latent) + mm(w.weh[...], hidden)
    target = target[: predicted.shape[0], :].astype(F32)
    return jnp.sum(predicted * (target - 0.5 * predicted), axis=0, keepdims=True)


def first_step(w, lat, ext_ref, c0_ref, put):
    sets = lat.shape[1] // BLK
    ext = jnp.concatenate([lat, jnp.concatenate([ext_ref[1]] * sets, axis=1)], axis=0)
    for c in range(CHUNKS):
        here = slice(c * w.rows, (c + 1) * w.rows)
        pre = [mm(w.wx[w.at(g, c), :], ext) for g in range(4)]
        before = c0_ref[here, :].astype(F32)
        put(here, *cell(pre, jnp.concatenate([before] * sets, axis=1)))


def later_step(w, hidden, ext, before, put):
    for c in range(CHUNKS):
        here = slice(c * w.rows, (c + 1) * w.rows)
        pre = [mm(w.wh[w.at(g, c), :], hidden) + mm(w.wx[w.at(g, c), :], ext) for g in range(4)]
        put(here, *cell(pre, before(here)))


def head(w, flags, source, me, off_ref, noise_ref, m1_ref, p1_ref, ext_ref, c0_ref, prior_ref, we_ref, h1, c1, l1):
    f0, f1 = flags[0] == 1, flags[1] == 1
    t = jnp.where(f0, 0, jnp.where(f1, 1, 2))
    d, cols = transition(t, source, off_ref, me)

    def gathered(k):
        return picked(d, cols, noise_ref[k], m1_ref[k], p1_ref[k])

    g0 = gathered(0)
    value = jnp.concatenate([jnp.where(f0, g0, noise_ref[0]), g0], axis=1)
    mean = jnp.concatenate([prior_ref[0]] * 2, axis=1)
    scale = jnp.concatenate([prior_ref[1]] * 2, axis=1)
    lat = (mean + scale * value).astype(BF16)

    def put(here, hidden, fresh):
        for k in range(2):
            h1[k, here, :] = hidden[:, k * BLK : (k + 1) * BLK]
            c1[k, here, :] = fresh[:, k * BLK : (k + 1) * BLK]

    first_step(w, lat, ext_ref, c0_ref, put)
    value = jnp.concatenate([noise_ref[1], jnp.where(f0, noise_ref[1], gathered(1))], axis=1)
    both = latents(w, jnp.concatenate([h1[0], h1[1]], axis=1), value)
    l1[0] = both[:, :BLK]
    l1[1] = both[:, BLK:]
    inc1 = increment(w, we_ref, ext_ref[2], l1[0], h1[0])
    lat0 = (prior_ref[0] + prior_ref[1] * noise_ref[0]).astype(BF16)
    nx = we_ref.shape[0]
    predicted = mm(we_ref[...], lat0) + prior_ref[2][:nx]
    inc0 = jnp.sum(predicted * (ext_ref[1][:nx].astype(F32) - 0.5 * predicted), axis=0, keepdims=True)
    return lat, inc0, inc1, d, cols


def tail(w, slot, value, inc0, inc1, flags, noise_ref, ext_ref, we_ref, h1, c1, l1, h2, c2, levels, out_ref, part_ref):
    hidden = jnp.concatenate([h1[slot], h1[1]], axis=1)
    latent = jnp.concatenate([l1[slot], l1[1]], axis=1)
    ext = jnp.concatenate([latent, jnp.concatenate([ext_ref[2]] * 2, axis=1)], axis=0)

    def before(here):
        return jnp.concatenate([c1[slot, here, :], c1[1, here, :]], axis=1).astype(F32)

    def put2(here, hidden, fresh):
        h2[here, :] = hidden
        c2[here, :] = fresh[:, BLK:]

    later_step(w, hidden, ext, before, put2)
    latent = latents(w, h2[...], jnp.concatenate([noise_ref[2], value], axis=1))
    ext = jnp.concatenate([latent[:, BLK:], ext_ref[3]], axis=0)

    def put3(here, hidden, fresh):
        out_ref[here, :] = hidden

    later_step(w, h2[:, BLK:], ext, lambda here: c2[here, :].astype(F32), put3)
    inc2 = increment(w, we_ref, ext_ref[3], latent[:, :BLK], h2[:, :BLK])
    latent = latents(w, out_ref[...], noise_ref[3])
    inc3 = increment(w, we_ref, ext_ref[4], latent, out_ref[...])
    weights = inc0
    levels[...] = jnp.zeros_like(levels)
    levels[0:1, :] = weights
    for t, inc in enumerate((inc1, inc2, inc3)):
        weights = jnp.where(flags[t] == 1, jnp.zeros_like(weights), weights) + inc
        levels[t + 1 : t + 2, :] = weights
    value = levels[...]
    peak = jnp.max(value, axis=1, keepdims=True)
    summed = jnp.sum(jnp.exp(value - peak), axis=1, keepdims=True)
    row = lax.broadcasted_iota(jnp.int32, (8, BLK), 0)
    lane = lax.broadcasted_iota(jnp.int32, (8, BLK), 1)
    line = jnp.where((row < 4) & (lane == row), peak, jnp.where((row < 4) & (lane == row + 4), summed, 0.0))
    line = jnp.sum(line, axis=0, keepdims=True)
    part_ref[...] = jnp.broadcast_to(line[None], part_ref.shape)


def one_kernel(
    flags, source, me_ref,
    wx, wh, wp, weh,
    off_ref, noise_ref, m1_ref, p1_ref, ext_ref, c0_ref, prior_ref, we_ref,
    out_ref, part_ref,
    h1, c1, l1, h2, c2, levels,
):
    w = Weights(wx, wh, wp, weh)
    _, inc0, inc1, d, cols = head(
        w, flags, source, me_ref[0], off_ref, noise_ref, m1_ref, p1_ref, ext_ref, c0_ref, prior_ref, we_ref, h1, c1, l1
    )
    g2 = picked(d, cols, noise_ref[2], m1_ref[2], p1_ref[2])
    value = jnp.where(flags[2] == 1, g2, noise_ref[2])
    slot = jnp.where(flags[1] == 1, 1, 0)
    tail(w, slot, value, inc0, inc1, flags, noise_ref, ext_ref, we_ref, h1, c1, l1, h2, c2, levels, out_ref, part_ref)


def early_kernel(
    flags, source, me_ref,
    wx, wh, wp, weh,
    off_ref, noise_ref, m1_ref, p1_ref, ext_ref, c0_ref, prior_ref, we_ref,
    h_ref, c_ref, msg_ref, inc_ref,
    h1, c1, l1,
):
    w = Weights(wx, wh, wp, weh)
    lat, inc0, inc1, _, _ = head(
        w, flags, source, me_ref[0], off_ref, noise_ref, m1_ref, p1_ref, ext_ref, c0_ref, prior_ref, we_ref, h1, c1, l1
    )
    h_ref[...] = h1[1]
    c_ref[...] = c1[1]
    msg_ref[0] = lat[:, BLK:]
    msg_ref[1] = l1[1]
    inc_ref[0:1, :] = inc0
    inc_ref[1:2, :] = inc1


def late_kernel(
    flags, source, me_ref,
    wx, wh, wp, weh,
    off_ref, noise_ref, m1_ref, p1_ref, ext_ref, c0_ref, we_ref,
    h_ref, c_ref, msg_ref, inc_ref, mm1_ref, mp1_ref,
    out_ref, part_ref,
    h1, c1, l1, h2, c2, levels,
):
    w = Weights(wx, wh, wp, weh)
    f2 = flags[2] == 1
    d, cols = transition(jnp.where(f2, 2, 1), source, off_ref, me_ref[0])
    lat = picked(d, cols, msg_ref[0], mm1_ref[0], mp1_ref[0]).astype(BF16)
    l1[1] = picked(d, cols, msg_ref[1], mm1_ref[1], mp1_ref[1]).astype(BF16)
    l1[0] = msg_ref[1]
    h1[0] = h_ref[...]
    c1[0] = c_ref[...]
    g2 = picked(d, cols, noise_ref[2], m1_ref[2], p1_ref[2])
    value = jnp.where(f2, g2, noise_ref[2])

    def put(here, hidden, fresh):
        h1[1, here, :] = hidden
        c1[1, here, :] = fresh

    first_step(w, lat, ext_ref, c0_ref, put)
    slot = jnp.where(f2, 0, 1)
    inc0, inc1 = inc_ref[0:1, :], inc_ref[1:2, :]
    tail(w, slot, value, inc0, inc1, flags, noise_ref, ext_ref, we_ref, h1, c1, l1, h2, c2, levels, out_ref, part_ref)


def bound_kernel(log_count, flags, part_ref, out_ref):
    pairs = part_ref[...].reshape(part_ref.shape[0], BLK)
    peaks = jnp.max(pairs, axis=0, keepdims=True)
    sums = pltpu.roll(pairs, BLK - 4, 1)
    summed = jnp.sum(sums * jnp.exp(pairs - peaks), axis=0, keepdims=True)
    lane = lax.broadcasted_iota(jnp.int32, (1, BLK), 1)
    used = lane == 3
    for t in range(3):
        used = used | ((lane == t) & (flags[t] == 1))
    levels = peaks + jnp.log(jnp.where(used, summed, 1.0)) - log_count
    out_ref[0] = jnp.sum(jnp.where(used, levels, 0.0))


def call(kernel, outs, spaces, scratch, args):
    return pl.pallas_call(
        kernel,
        name=kernel.__name__,
        out_shape=outs,
        in_specs=[pl.BlockSpec(memory_space=s) for s in spaces],
        out_specs=[pl.BlockSpec(memory_space=SM if o.shape == (1,) else VM) for o in outs],
        scratch_shapes=scratch,
        compiler_params=pltpu.CompilerParams(vmem_limit_bytes=LIMIT),
    )(*args)


def body(
    observed, latent_noise, w_hidden, w_latent, w_frame, gate_bias, w_prior, w_emit, w_emit_hidden,
    block_source, inner_offset, resample_flags,
):
    count = lax.axis_size("dom")
    width = w_hidden.shape[1]
    nx = w_emit.shape[0]
    steps = latent_noise.shape[0]
    sds = jax.ShapeDtypeStruct

    def swapped(value, first):
        pairs = [(i, i + 1) for i in range(first, count - 1, 2)]
        return lax.ppermute(value, "dom", pairs + [(b, a) for a, b in pairs])

    def exchanged(value):
        odd = swapped(value, 1)
        return swapped(value, 0), odd

    halos = exchanged(latent_noise)
    wh, wx, ext, c0, prior, wp, weh, moves_twice = call(
        start_kernel,
        [
            sds(w_hidden.shape, BF16),
            sds((4 * width, 2 * BLK), BF16),
            sds((steps + 1, BLK, BLK), BF16),
            sds((width, BLK), BF16),
            sds((3, BLK, BLK), F32),
            sds(w_prior.shape, BF16),
            sds(w_emit_hidden.shape, BF16),
            sds((1,), jnp.int32),
        ],
        [SM] + [HBM] * 7,
        [
            pltpu.VMEM((nx, 4 * width), BF16),
            pltpu.VMEM((BLK, 4 * width), F32),
            pltpu.VMEM((BLK, BLK), F32),
            pltpu.VMEM((steps + 1, nx), BF16),
            pltpu.VMEM((1, 4 * width), F32),
            pltpu.SemaphoreType.DMA((6 + PIECES,)),
        ],
        (
            resample_flags,
            *(
                pltpu.with_memory_space_constraint(v, HBM)
                for v in (
                    observed, gate_bias.reshape(1, -1), w_frame, w_latent, w_prior, w_emit_hidden, w_hidden,
                )
            ),
        ),
    )
    me = lax.axis_index("dom").astype(jnp.int32).reshape(1)
    outs = [sds((width, BLK), BF16), sds((count, 1, BLK), F32)]
    states = [
        pltpu.VMEM((2, width, BLK), BF16),
        pltpu.VMEM((2, width, BLK), BF16),
        pltpu.VMEM((2, BLK, BLK), BF16),
    ]
    rest = [
        pltpu.VMEM((width, 2 * BLK), BF16),
        pltpu.VMEM((width, BLK), BF16),
        pltpu.VMEM((8, BLK), F32),
    ]
    scalars = (resample_flags, block_source, me)
    shared = (inner_offset, latent_noise, *halos, ext, c0)

    def once():
        return call(
            one_kernel, outs, [SM] * 3 + [VM] * 12, [*states, *rest],
            (*scalars, wx, wh, wp, weh, *shared, prior, w_emit),
        )

    def twice():
        h_kept, c_kept, msg, incs = call(
            early_kernel,
            [sds((width, BLK), BF16), sds((width, BLK), BF16), sds((2, BLK, BLK), BF16), sds((8, BLK), F32)],
            [SM] * 3 + [VM] * 12, states,
            (*scalars, wx, wh, wp, weh, *shared, prior, w_emit),
        )
        return call(
            late_kernel, outs, [SM] * 3 + [VM] * 17, [*states, *rest],
            (
                *scalars, wx, wh, wp, weh, *shared, w_emit,
                h_kept, c_kept, msg, incs, *exchanged(msg),
            ),
        )

    hidden, part = lax.cond(moves_twice[0] == 1, twice, once)
    parts = lax.all_to_all(part, "dom", 0, 0, tiled=True)
    bound = pl.pallas_call(
        partial(bound_kernel, math.log(BLK * count)),
        name="bound",
        out_shape=sds((1,), F32),
        in_specs=[pl.BlockSpec(memory_space=SM), pl.BlockSpec(memory_space=VM)],
        out_specs=pl.BlockSpec(memory_space=SM),
        compiler_params=pltpu.CompilerParams(vmem_limit_bytes=LIMIT),
    )(resample_flags, parts)
    return hidden, bound


def solution(mesh):
    in_specs = (
        P("seq", None),
        P(None, None, ("seq", "dom")),
        P(),
        P(),
        P(),
        P(),
        P(),
        P(),
        P(),
        P("seq", None),
        P("seq", None),
        P(),
    )
    out_specs = (P(None, ("seq", "dom")), P("seq"))
    return jax.shard_map(body, mesh=mesh, in_specs=in_specs, out_specs=out_specs, check_vma=False)
```

```python
from functools import partial
import math

import jax
import jax.numpy as jnp
from jax import lax
from jax.experimental import pallas as pl
from jax.experimental.pallas import tpu as pltpu
from jax.sharding import PartitionSpec as P


BLK = 128
CHUNKS = 2
PIECES = 4
F32 = jnp.float32
BF16 = jnp.bfloat16
VM, SM, HBM = pltpu.VMEM, pltpu.SMEM, pltpu.HBM
LIMIT = 8 << 20


def sigmoid(x):
    return 0.5 * jnp.tanh(0.5 * x) + 0.5


def mm(a, b):
    return jnp.dot(a, b, preferred_element_type=F32)


def mm_rows(a, b):
    return lax.dot_general(a, b, (((1,), (1,)), ((), ())), preferred_element_type=F32)


def three_parts(x):
    hi = x.astype(BF16)
    rest = x - hi.astype(F32)
    mid = rest.astype(BF16)
    return hi, mid, (rest - mid.astype(F32)).astype(BF16)


def column(row):
    return jnp.broadcast_to(row, (BLK, BLK)).T


def start_kernel(
    flags, obs_hbm, bias_hbm, wf_hbm, wl_hbm, wp_hbm, weh_hbm, wh_hbm,
    wh, wx_ref, ext_ref, c0_ref, prior_ref, wp, weh, twice_ref,
    wf, tmp, square, obs, bias, sems,
):
    width = c0_ref.shape[0]
    pieces = sems.shape[0] - 6
    rows = 4 * width // pieces
    nx = wf.shape[0]
    pairs = [(obs_hbm, obs), (bias_hbm, bias), (wf_hbm, wf), (wp_hbm, wp), (weh_hbm, weh)]
    pairs += [(wh_hbm.at[pl.ds(c * rows, rows)], wh.at[pl.ds(c * rows, rows)]) for c in range(pieces)]
    pairs += [(wl_hbm, wx_ref.at[:, pl.ds(0, BLK)])]
    copies = [pltpu.make_async_copy(a, b, sems.at[k]) for k, (a, b) in enumerate(pairs)]
    for copy in copies:
        copy.start()
    twice_ref[0] = jnp.where(flags[0] + flags[1] + flags[2] == 2, 1, 0)
    lane = lax.broadcasted_iota(jnp.int32, (BLK, BLK), 1)
    row = lax.broadcasted_iota(jnp.int32, (BLK, BLK), 0)
    for copy in copies[:2]:
        copy.wait()
    square[...] = jnp.where((lane >= nx) & (lane < nx + 3), 1.0, 0.0)
    square[0:5, 0:nx] = obs[...].astype(F32)
    tmp[nx:, :] = jnp.zeros((BLK - nx, tmp.shape[1]), F32)
    for k, part in enumerate(three_parts(bias[...])):
        tmp[nx + k : nx + k + 1, :] = part.astype(F32)
    obs_cols = square[...].T
    for t in range(1, ext_ref.shape[0]):
        value = jnp.broadcast_to(obs_cols[:, t : t + 1], (BLK, BLK))
        if t == 1:
            value = jnp.where((row >= nx + 3) & (row < nx + 6), 1.0, value)
        ext_ref[t] = value.astype(BF16)

    copies[2].wait()
    frame = mm(square[0:8, 0:nx].astype(BF16), wf[...])[0:1]
    gates = frame + bias[...]
    fresh = sigmoid(gates[:, 0:width]) * jnp.tanh(gates[:, 2 * width : 3 * width])
    hidden = (sigmoid(gates[:, 3 * width :]) * jnp.tanh(fresh)).astype(BF16)
    fresh = fresh.astype(BF16).astype(F32)
    hidden8 = jnp.broadcast_to(hidden.astype(F32), (8, width)).astype(BF16)
    for copy in copies[3:5]:
        copy.wait()
    prior = mm_rows(hidden8, wp[...])[0:1]
    shared = mm_rows(hidden8, weh[...])[0:1]
    shared = jnp.concatenate([shared, jnp.zeros((1, BLK - nx), F32)], axis=1)
    tmp[0:nx, :] = wf[...].astype(F32)
    for r in range(width // BLK):
        c0_ref[r * BLK : (r + 1) * BLK, :] = column(fresh[:, r * BLK : (r + 1) * BLK]).astype(BF16)
    prior_ref[0] = column(prior[:, :BLK])
    prior_ref[1] = column(jnp.exp(0.5 * jnp.tanh(prior[:, BLK:])))
    prior_ref[2] = column(shared)
    for c in range(pieces):
        copies[5 + c].wait()
        here = slice(c * rows, (c + 1) * rows)
        moved = mm_rows(hidden8, wh[here, :])[0:1]
        for k, part in enumerate(three_parts(moved)):
            tmp[nx + 3 + k : nx + 4 + k, here] = part.astype(F32)
        for r in range(c * rows // BLK, (c + 1) * rows // BLK):
            wx_ref[r * BLK : (r + 1) * BLK, BLK:] = tmp[:, r * BLK : (r + 1) * BLK].T.astype(BF16)
    copies[-1].wait()


def take(x, idx):
    idx = jnp.broadcast_to(idx[0:1], x.shape)
    return jnp.take_along_axis(x, idx, axis=1, mode="promise_in_bounds")


def transition(t, source, off_ref, me):
    last = off_ref.shape[1] // BLK - 1
    at = jnp.clip(source[t, me], 0, last)
    start = pl.multiple_of(me * BLK, BLK)
    cols = jnp.where(t == 2, off_ref[2:3, pl.ds(start, BLK)], off_ref[1:2, pl.ds(start, BLK)])
    cols = jnp.where(t == 0, off_ref[0:1, pl.ds(start, BLK)], cols)
    d = at - me
    partner = jnp.where(d == 0, 0, jnp.where((d == 1) == (lax.rem(me, 2) == 0), 1, 2))
    return partner, jnp.broadcast_to(cols, (8, BLK))


def picked(partner, cols, own, even, odd):
    value = jnp.where(partner == 1, even.astype(F32), jnp.where(partner == 2, odd.astype(F32), own.astype(F32)))
    return take(value, cols)


def cell(pre, cell_state):
    fresh = sigmoid(pre[1]) * cell_state + sigmoid(pre[0]) * jnp.tanh(pre[2])
    return (sigmoid(pre[3]) * jnp.tanh(fresh)).astype(BF16), fresh.astype(BF16)


class Weights:
    def __init__(self, wx, wh, wp, weh):
        self.wx, self.wh, self.wp, self.weh = wx, wh, wp, weh
        self.width = wx.shape[0] // 4
        self.rows = self.width // CHUNKS

    def at(self, g, c):
        start = g * self.width + c * self.rows
        return slice(start, start + self.rows)


def latents(w, hidden, value):
    prior = mm(w.wp[...], hidden)
    return (prior[:BLK] + jnp.exp(0.5 * jnp.tanh(prior[BLK:])) * value).astype(BF16)


def increment(w, we_ref, target, latent, hidden):
    predicted = mm(we_ref[...], latent) + mm(w.weh[...], hidden)
    target = target[: predicted.shape[0], :].astype(F32)
    return jnp.sum(predicted * (target - 0.5 * predicted), axis=0, keepdims=True)


def first_step(w, lat, ext_ref, c0_ref, put):
    sets = lat.shape[1] // BLK
    ext = jnp.concatenate([lat, jnp.concatenate([ext_ref[1]] * sets, axis=1)], axis=0)
    for c in range(CHUNKS):
        here = slice(c * w.rows, (c + 1) * w.rows)
        pre = [mm(w.wx[w.at(g, c), :], ext) for g in range(4)]
        before = c0_ref[here, :].astype(F32)
        put(here, *cell(pre, jnp.concatenate([before] * sets, axis=1)))


def later_step(w, hidden, ext, before, put):
    for c in range(CHUNKS):
        here = slice(c * w.rows, (c + 1) * w.rows)
        pre = [mm(w.wh[w.at(g, c), :], hidden) + mm(w.wx[w.at(g, c), :], ext) for g in range(4)]
        put(here, *cell(pre, before(here)))


def head(w, flags, source, me, off_ref, noise_ref, m1_ref, p1_ref, ext_ref, c0_ref, prior_ref, we_ref, h1, c1, l1):
    f0, f1 = flags[0] == 1, flags[1] == 1
    t = jnp.where(f0, 0, jnp.where(f1, 1, 2))
    d, cols = transition(t, source, off_ref, me)

    def gathered(k):
        return picked(d, cols, noise_ref[k], m1_ref[k], p1_ref[k])

    g0 = gathered(0)
    value = jnp.concatenate([jnp.where(f0, g0, noise_ref[0]), g0], axis=1)
    mean = jnp.concatenate([prior_ref[0]] * 2, axis=1)
    scale = jnp.concatenate([prior_ref[1]] * 2, axis=1)
    lat = (mean + scale * value).astype(BF16)

    def put(here, hidden, fresh):
        for k in range(2):
            h1[k, here, :] = hidden[:, k * BLK : (k + 1) * BLK]
            c1[k, here, :] = fresh[:, k * BLK : (k + 1) * BLK]

    first_step(w, lat, ext_ref, c0_ref, put)
    value = jnp.concatenate([noise_ref[1], jnp.where(f0, noise_ref[1], gathered(1))], axis=1)
    both = latents(w, jnp.concatenate([h1[0], h1[1]], axis=1), value)
    l1[0] = both[:, :BLK]
    l1[1] = both[:, BLK:]
    inc1 = increment(w, we_ref, ext_ref[2], l1[0], h1[0])
    lat0 = (prior_ref[0] + prior_ref[1] * noise_ref[0]).astype(BF16)
    nx = we_ref.shape[0]
    predicted = mm(we_ref[...], lat0) + prior_ref[2][:nx]
    inc0 = jnp.sum(predicted * (ext_ref[1][:nx].astype(F32) - 0.5 * predicted), axis=0, keepdims=True)
    return lat, inc0, inc1, d, cols


def tail(w, slot, value, inc0, inc1, flags, noise_ref, ext_ref, we_ref, h1, c1, l1, h2, c2, levels, out_ref, part_ref):
    hidden = jnp.concatenate([h1[slot], h1[1]], axis=1)
    latent = jnp.concatenate([l1[slot], l1[1]], axis=1)
    ext = jnp.concatenate([latent, jnp.concatenate([ext_ref[2]] * 2, axis=1)], axis=0)

    def before(here):
        return jnp.concatenate([c1[slot, here, :], c1[1, here, :]], axis=1).astype(F32)

    def put2(here, hidden, fresh):
        h2[here, :] = hidden
        c2[here, :] = fresh[:, BLK:]

    later_step(w, hidden, ext, before, put2)
    latent = latents(w, h2[...], jnp.concatenate([noise_ref[2], value], axis=1))
    ext = jnp.concatenate([latent[:, BLK:], ext_ref[3]], axis=0)

    def put3(here, hidden, fresh):
        out_ref[here, :] = hidden

    later_step(w, h2[:, BLK:], ext, lambda here: c2[here, :].astype(F32), put3)
    inc2 = increment(w, we_ref, ext_ref[3], latent[:, :BLK], h2[:, :BLK])
    latent = latents(w, out_ref[...], noise_ref[3])
    inc3 = increment(w, we_ref, ext_ref[4], latent, out_ref[...])
    weights = inc0
    levels[...] = jnp.zeros_like(levels)
    levels[0:1, :] = weights
    for t, inc in enumerate((inc1, inc2, inc3)):
        weights = jnp.where(flags[t] == 1, jnp.zeros_like(weights), weights) + inc
        levels[t + 1 : t + 2, :] = weights
    value = levels[...]
    peak = jnp.max(value, axis=1, keepdims=True)
    summed = jnp.sum(jnp.exp(value - peak), axis=1, keepdims=True)
    row = lax.broadcasted_iota(jnp.int32, (8, BLK), 0)
    lane = lax.broadcasted_iota(jnp.int32, (8, BLK), 1)
    line = jnp.where((row < 4) & (lane == row), peak, jnp.where((row < 4) & (lane == row + 4), summed, 0.0))
    line = jnp.sum(line, axis=0, keepdims=True)
    part_ref[...] = jnp.broadcast_to(line[None], part_ref.shape)


def one_kernel(
    flags, source, me_ref,
    wx, wh, wp, weh,
    off_ref, noise_ref, m1_ref, p1_ref, ext_ref, c0_ref, prior_ref, we_ref,
    out_ref, part_ref,
    h1, c1, l1, h2, c2, levels,
):
    w = Weights(wx, wh, wp, weh)
    _, inc0, inc1, d, cols = head(
        w, flags, source, me_ref[0], off_ref, noise_ref, m1_ref, p1_ref, ext_ref, c0_ref, prior_ref, we_ref, h1, c1, l1
    )
    g2 = picked(d, cols, noise_ref[2], m1_ref[2], p1_ref[2])
    value = jnp.where(flags[2] == 1, g2, noise_ref[2])
    slot = jnp.where(flags[1] == 1, 1, 0)
    tail(w, slot, value, inc0, inc1, flags, noise_ref, ext_ref, we_ref, h1, c1, l1, h2, c2, levels, out_ref, part_ref)


def early_kernel(
    flags, source, me_ref,
    wx, wh, wp, weh,
    off_ref, noise_ref, m1_ref, p1_ref, ext_ref, c0_ref, prior_ref, we_ref,
    h_ref, c_ref, msg_ref, inc_ref,
    h1, c1, l1,
):
    w = Weights(wx, wh, wp, weh)
    lat, inc0, inc1, _, _ = head(
        w, flags, source, me_ref[0], off_ref, noise_ref, m1_ref, p1_ref, ext_ref, c0_ref, prior_ref, we_ref, h1, c1, l1
    )
    h_ref[...] = h1[1]
    c_ref[...] = c1[1]
    msg_ref[0] = lat[:, BLK:]
    msg_ref[1] = l1[1]
    inc_ref[0:1, :] = inc0
    inc_ref[1:2, :] = inc1


def late_kernel(
    flags, source, me_ref,
    wx, wh, wp, weh,
    off_ref, noise_ref, m1_ref, p1_ref, ext_ref, c0_ref, we_ref,
    h_ref, c_ref, msg_ref, inc_ref, mm1_ref, mp1_ref,
    out_ref, part_ref,
    h1, c1, l1, h2, c2, levels,
):
    w = Weights(wx, wh, wp, weh)
    f2 = flags[2] == 1
    d, cols = transition(jnp.where(f2, 2, 1), source, off_ref, me_ref[0])
    lat = picked(d, cols, msg_ref[0], mm1_ref[0], mp1_ref[0]).astype(BF16)
    l1[1] = picked(d, cols, msg_ref[1], mm1_ref[1], mp1_ref[1]).astype(BF16)
    l1[0] = msg_ref[1]
    h1[0] = h_ref[...]
    c1[0] = c_ref[...]
    g2 = picked(d, cols, noise_ref[2], m1_ref[2], p1_ref[2])
    value = jnp.where(f2, g2, noise_ref[2])

    def put(here, hidden, fresh):
        h1[1, here, :] = hidden
        c1[1, here, :] = fresh

    first_step(w, lat, ext_ref, c0_ref, put)
    slot = jnp.where(f2, 0, 1)
    inc0, inc1 = inc_ref[0:1, :], inc_ref[1:2, :]
    tail(w, slot, value, inc0, inc1, flags, noise_ref, ext_ref, we_ref, h1, c1, l1, h2, c2, levels, out_ref, part_ref)


def bound_kernel(log_count, flags, part_ref, out_ref):
    pairs = part_ref[...].reshape(part_ref.shape[0], BLK)
    peaks = jnp.max(pairs, axis=0, keepdims=True)
    sums = pltpu.roll(pairs, BLK - 4, 1)
    summed = jnp.sum(sums * jnp.exp(pairs - peaks), axis=0, keepdims=True)
    lane = lax.broadcasted_iota(jnp.int32, (1, BLK), 1)
    used = lane == 3
    for t in range(3):
        used = used | ((lane == t) & (flags[t] == 1))
    levels = peaks + jnp.log(jnp.where(used, summed, 1.0)) - log_count
    out_ref[0] = jnp.sum(jnp.where(used, levels, 0.0))


def call(kernel, outs, spaces, scratch, args):
    return pl.pallas_call(
        kernel,
        out_shape=outs,
        in_specs=[pl.BlockSpec(memory_space=s) for s in spaces],
        out_specs=[pl.BlockSpec(memory_space=SM if o.shape == (1,) else VM) for o in outs],
        scratch_shapes=scratch,
        compiler_params=pltpu.CompilerParams(vmem_limit_bytes=LIMIT),
    )(*args)


def body(
    observed, latent_noise, w_hidden, w_latent, w_frame, gate_bias, w_prior, w_emit, w_emit_hidden,
    block_source, inner_offset, resample_flags,
):
    count = lax.axis_size("dom")
    width = w_hidden.shape[1]
    nx = w_emit.shape[0]
    steps = latent_noise.shape[0]
    sds = jax.ShapeDtypeStruct

    def swapped(value, first):
        pairs = [(i, i + 1) for i in range(first, count - 1, 2)]
        return lax.ppermute(value, "dom", pairs + [(b, a) for a, b in pairs])

    def exchanged(value):
        odd = swapped(value, 1)
        even = swapped(value, 0)
        return even, odd

    halos = exchanged(latent_noise)
    wh, wx, ext, c0, prior, wp, weh, moves_twice = call(
        start_kernel,
        [
            sds(w_hidden.shape, BF16),
            sds((4 * width, 2 * BLK), BF16),
            sds((steps + 1, BLK, BLK), BF16),
            sds((width, BLK), BF16),
            sds((3, BLK, BLK), F32),
            sds(w_prior.shape, BF16),
            sds(w_emit_hidden.shape, BF16),
            sds((1,), jnp.int32),
        ],
        [SM] + [HBM] * 7,
        [
            pltpu.VMEM((nx, 4 * width), BF16),
            pltpu.VMEM((BLK, 4 * width), F32),
            pltpu.VMEM((BLK, BLK), F32),
            pltpu.VMEM((steps + 1, nx), BF16),
            pltpu.VMEM((1, 4 * width), F32),
            pltpu.SemaphoreType.DMA((6 + PIECES,)),
        ],
        (
            resample_flags,
            *(
                pltpu.with_memory_space_constraint(v, HBM)
                for v in (
                    observed, gate_bias.reshape(1, -1), w_frame, w_latent, w_prior, w_emit_hidden, w_hidden,
                )
            ),
        ),
    )
    me = lax.axis_index("dom").astype(jnp.int32).reshape(1)
    outs = [sds((width, BLK), BF16), sds((count, 1, BLK), F32)]
    states = [
        pltpu.VMEM((2, width, BLK), BF16),
        pltpu.VMEM((2, width, BLK), BF16),
        pltpu.VMEM((2, BLK, BLK), BF16),
    ]
    rest = [
        pltpu.VMEM((width, 2 * BLK), BF16),
        pltpu.VMEM((width, BLK), BF16),
        pltpu.VMEM((8, BLK), F32),
    ]
    scalars = (resample_flags, block_source, me)
    shared = (inner_offset, latent_noise, *halos, ext, c0)

    def once():
        return call(
            one_kernel, outs, [SM] * 3 + [VM] * 12, [*states, *rest],
            (*scalars, wx, wh, wp, weh, *shared, prior, w_emit),
        )

    def twice():
        h_kept, c_kept, msg, incs = call(
            early_kernel,
            [sds((width, BLK), BF16), sds((width, BLK), BF16), sds((2, BLK, BLK), BF16), sds((8, BLK), F32)],
            [SM] * 3 + [VM] * 12, states,
            (*scalars, wx, wh, wp, weh, *shared, prior, w_emit),
        )
        return call(
            late_kernel, outs, [SM] * 3 + [VM] * 17, [*states, *rest],
            (
                *scalars, wx, wh, wp, weh, *shared, w_emit,
                h_kept, c_kept, msg, incs, *exchanged(msg),
            ),
        )

    hidden, part = lax.cond(moves_twice[0] == 1, twice, once)
    parts = lax.all_to_all(part, "dom", 0, 0, tiled=True)
    bound = pl.pallas_call(
        partial(bound_kernel, math.log(BLK * count)),
        name="bound",
        out_shape=sds((1,), F32),
        in_specs=[pl.BlockSpec(memory_space=SM), pl.BlockSpec(memory_space=VM)],
        out_specs=pl.BlockSpec(memory_space=SM),
        compiler_params=pltpu.CompilerParams(vmem_limit_bytes=LIMIT),
    )(resample_flags, parts)
    return hidden, bound


def solution(mesh):
    in_specs = (
        P("seq", None),
        P(None, None, ("seq", "dom")),
        P(),
        P(),
        P(),
        P(),
        P(),
        P(),
        P(),
        P("seq", None),
        P("seq", None),
        P(),
    )
    out_specs = (P(None, ("seq", "dom")), P("seq"))
    return jax.shard_map(body, mesh=mesh, in_specs=in_specs, out_specs=out_specs, check_vma=False)
```
